32 devices in a mesh: gx: 4 (over x, core), gy: 4 (over z), gz: 2 (over y).
Axes of the slice: x: 2, y: 2, z: 4, core: 2. Of those that a mesh axis runs over, the one named last changes fastest.
Arguments:
- orbitals: float32 [64, 32, 32, 256], P(None, 'gx', 'gy', 'gz'), may hold values from -6 to 6
- potential: float32 [32, 32, 256], P('gx', 'gy', 'gz'), may hold values from 0 to 0.5
- centre: float32 [64], replicated, may hold values from 3 to 5
- half_width: float32 [64], replicated, may hold values from 3 to 5
Outputs:
- filtered: float32 [64, 32, 32, 256], P(None, 'gx', 'gy', 'gz')
The draws below stay inside these ranges and needn't reach their ends.
All inputs are finite; a program needn't handle non-finite values.
Results may differ from the reference program's by a relative error of at most 0.00002.
Values sent between devices are 32-bit elements; how exact they have to be, the bound alone decides.
A program may use at most 64 MiB of HBM per device.

```python
import jax
import jax.numpy as jnp
from jax import lax

BANDS = 64
NX = 32
NY = 32
NZ = 256


def block_levels(rng, shape, split, least, top_value):
    def one(axis_at, blocks):
        heights = jax.random.uniform(jax.random.fold_in(jax.random.fold_in(rng, 6), axis_at), (blocks,), jnp.float32, least / len(split), top_value / len(split))
        return jnp.repeat(jnp.exp(heights), shape[axis_at] // blocks).reshape((-1,) + (1,) * (len(shape) - axis_at - 1))

    level = one(*split[0])
    for cut in split[1:]:
        level = level * one(*cut)
    return level


def gaussian(stream_key, dims, scale, bound, split=(), dtype=jnp.bfloat16):
    result = jax.random.normal(stream_key, dims, jnp.float32) * scale
    if len(split) > 0:
        result = block_levels(stream_key, dims, split, -0.22, 0.18) * result
    return jnp.clip(result, min=-bound, max=bound).astype(dtype)


def setup_inputs(seed: int = 0) -> dict:
    key_of = jax.random.split(jax.random.key(seed), 5)
    orbitals = gaussian(key_of[0], (BANDS, NX, NY, NZ), 1.0, 6.0, ((1, 4), (2, 4), (3, 2)), jnp.float32)
    potential = jnp.clip(0.5 * jax.random.uniform(key_of[1], (NX, NY, NZ), jnp.float32) ** block_levels(key_of[1], (NX, NY, NZ), ((0, 4), (1, 4), (2, 2)), -0.2, 0.2), 0.0, 0.5)
    centre = jnp.clip(jax.random.uniform(key_of[2], (BANDS,), jnp.float32, 3.0, 5.0), 3.0, 5.0)
    half_width = jnp.clip(jax.random.uniform(key_of[3], (BANDS,), jnp.float32, 3.0, 5.0), 3.0, 5.0)
    return {"orbitals": orbitals, "potential": potential, "centre": centre, "half_width": half_width}


shift_mass = 0.05
jacobi_weight = 2.0 / 3.0


def neighbour_sum(field):
    total = jnp.roll(field, 1, 0) + jnp.roll(field, -1, 0)
    total = total + jnp.roll(field, 1, 1) + jnp.roll(field, -1, 1)
    return total + jnp.roll(field, 1, 2) + jnp.roll(field, -1, 2)


def operate(field, diagonal, coupling):
    return diagonal * field - coupling * neighbour_sum(field)


def restrict(field):
    shape = field.shape
    return 0.5 * field.reshape(shape[0] // 2, 2, shape[1] // 2, 2, shape[2] // 2, 2).sum(axis=(1, 3, 5))


def average_cells(field):
    shape = field.shape
    return 0.125 * field.reshape(shape[0] // 2, 2, shape[1] // 2, 2, shape[2] // 2, 2).sum(axis=(1, 3, 5))


def prolong(field):
    return jnp.repeat(jnp.repeat(jnp.repeat(field, 2, 0), 2, 1), 2, 2)


def relax(level, source, diagonal, coupling):
    return level + jacobi_weight * (source - operate(level, diagonal, coupling)) / diagonal


def reference(orbitals, potential, centre, half_width):
    potential_one = average_cells(potential)
    potential_two = average_cells(potential_one)
    diagonal_fine = 3.0 + potential
    diagonal_one = 0.75 + potential_one + shift_mass
    diagonal_two = 0.1875 + potential_two + shift_mass

    def one_band(packed):
        orbital, middle, spread = packed
        first_image = operate(orbital, diagonal_fine, 0.5)
        first_order = (first_image - middle * orbital) / spread
        second_image = operate(first_order, diagonal_fine, 0.5)
        second_order = 2.0 * (second_image - middle * first_order) / spread - orbital
        source_one = restrict(second_order)
        level_one = jacobi_weight * source_one / diagonal_one
        level_one = relax(level_one, source_one, diagonal_one, 0.125)
        residue = source_one - operate(level_one, diagonal_one, 0.125)
        source_two = restrict(residue)
        level_two = jacobi_weight * source_two / diagonal_two
        for sweep_index in range(2):
            level_two = relax(level_two, source_two, diagonal_two, 0.03125)
        level_one = level_one + prolong(level_two)
        level_one = relax(level_one, source_one, diagonal_one, 0.125)
        return second_order + prolong(level_one)

    return lax.map(one_band, (orbitals, centre, half_width))
```

```python
import functools

import jax
import jax.numpy as jnp
from jax import lax
from jax.experimental import pallas as pl
from jax.experimental.pallas import tpu as pltpu
from jax.sharding import PartitionSpec as P

shift_mass = 0.05
jacobi_weight = 2.0 / 3.0
MESH = pl.DeviceIdType.MESH
ORB, FIRST = range(2)


def kernel(sizes, chunks, centre_in, half_width_in, pot_in, orbitals, out, *scratch):
    fine = scratch[0:2]
    one_a, one_b, two_a, two_b, two_c = scratch[2:7]
    second, zsend, zrecv = scratch[7:10]
    one_edge, one_got, one_halo, two_edge, two_got, last_edge, last_got = scratch[10:17]
    band_a, band_i, pot_b, d1_b, r1_b, r2_b, r_sent, r_got = scratch[17:25]
    load_sem, store_sem, fine_sem, one_sem, two_sem, last_sem, r_sem = scratch[25:32]
    centre, half_width, pot, small_sem = scratch[32:36]
    bands, nx, ny, nz = second.shape[2], second.shape[0], second.shape[1], second.shape[3]
    width = bands // chunks
    groups = width // 8
    pairs = chunks // 2
    mx, my, qx, qy = nx // 2, ny // 2, nx // 4, ny // 4
    sides = 2 if sizes["gz"] > 2 else 1
    lane = lax.broadcasted_iota(jnp.int32, (8, nz), 1)
    sub = lax.broadcasted_iota(jnp.int32, (8, nz), 0)

    near = {}
    for axis in ("gx", "gy", "gz"):
        me, n = lax.axis_index(axis), sizes[axis]
        near[axis] = (lax.rem(me + n - 1, n), lax.rem(me + 1, n))
    zpeers = [near["gz"][1], near["gz"][0]][:sides]
    peers = [{"gx": v} for v in near["gx"]] + [{"gy": v} for v in near["gy"]]
    peers += [{"gz": v} for v in zpeers]

    barrier = pltpu.get_barrier_semaphore()
    for peer in peers:
        pl.semaphore_signal(barrier, inc=1, device_id=peer, device_id_type=MESH)

    smalls = [
        pltpu.make_async_copy(src, dst, small_sem.at[j])
        for j, (src, dst) in enumerate(
            [(centre_in, centre), (half_width_in, half_width), (pot_in, pot)]
        )
    ]
    for small in smalls:
        small.start()

    def loads(k):
        rows = pl.ds(pl.multiple_of(k * width, 8), width)

        def line(x, _):
            for y in range(ny):
                pltpu.make_async_copy(
                    orbitals.at[rows, x, y], fine[ORB].at[x + 1, y + 1, rows], load_sem.at[k]
                ).start()
            return 0

        lax.fori_loop(0, nx, line, 0)

    lax.fori_loop(0, chunks, lambda k, c: (loads(k), c)[1], 0)

    def remote(moves, sems, at):
        return [
            pltpu.make_async_remote_copy(
                src_ref=src,
                dst_ref=dst,
                send_sem=sems.at[(0, *at, j)],
                recv_sem=sems.at[(1, *at, j)],
                device_id=to,
                device_id_type=MESH,
            )
            for j, (src, dst, to) in enumerate(moves)
        ]

    def fine_moves(p, k):
        e = fine[p]
        rows = pl.ds(pl.multiple_of(k * width, 8), width)
        ys, xs = pl.ds(1, ny), pl.ds(1, nx)
        moves = [
            (e.at[xs, 1, rows], e.at[xs, ny + 1, rows], {"gy": near["gy"][0]}),
            (e.at[xs, ny, rows], e.at[xs, 0, rows], {"gy": near["gy"][1]}),
            (e.at[1, ys, rows], e.at[nx + 1, ys, rows], {"gx": near["gx"][0]}),
            (e.at[nx, ys, rows], e.at[0, ys, rows], {"gx": near["gx"][1]}),
        ]
        for s, to in enumerate(zpeers):
            moves.append((zsend.at[p, rows], zrecv.at[p, s, rows], {"gz": to}))
        return remote(moves, fine_sem, (p, k))

    def deep_moves(e, edge, got, sems, k):
        ax, ay = e.shape[0] - 4, e.shape[1] - 4
        rows = pl.ds(pl.multiple_of(k * 8, 8), 8)
        ys, xs = pl.ds(2, ay), pl.ds(2, ax)
        lo, hix, hiy, topx, topy = pl.ds(0, 2), pl.ds(ax, 2), pl.ds(ay, 2), pl.ds(ax + 2, 2), pl.ds(ay + 2, 2)
        two = pl.ds(2, 2)
        (xm, xp), (ym, yp) = near["gx"], near["gy"]
        moves = [
            (e.at[xs, two, rows], e.at[xs, topy, rows], {"gy": ym}),
            (e.at[xs, hiy, rows], e.at[xs, lo, rows], {"gy": yp}),
            (e.at[two, ys, rows], e.at[topx, ys, rows], {"gx": xm}),
            (e.at[hix, ys, rows], e.at[lo, ys, rows], {"gx": xp}),
            (e.at[2, 2, rows], e.at[ax + 2, ay + 2, rows], {"gx": xm, "gy": ym}),
            (e.at[ax + 1, 2, rows], e.at[1, ay + 2, rows], {"gx": xp, "gy": ym}),
            (e.at[2, ay + 1, rows], e.at[ax + 2, 1, rows], {"gx": xm, "gy": yp}),
            (e.at[ax + 1, ay + 1, rows], e.at[1, 1, rows], {"gx": xp, "gy": yp}),
        ]
        for s, z in enumerate(zpeers):
            for j, to in enumerate([{}, {"gx": xp}, {"gx": xm}, {"gy": yp}, {"gy": ym}]):
                moves.append((edge.at[rows], got.at[s, j, rows], {"gz": z, **to}))
        return remote(moves, sems, (k,))

    def last_moves(k):
        e = two_c
        rows = pl.ds(pl.multiple_of(k * 8, 8), 8)
        ys, xs = pl.ds(1, qy), pl.ds(1, qx)
        moves = [
            (e.at[xs, 1, rows], e.at[xs, qy + 1, rows], {"gy": near["gy"][0]}),
            (e.at[xs, qy, rows], e.at[xs, 0, rows], {"gy": near["gy"][1]}),
            (e.at[1, ys, rows], e.at[qx + 1, ys, rows], {"gx": near["gx"][0]}),
            (e.at[qx, ys, rows], e.at[0, ys, rows], {"gx": near["gx"][1]}),
        ]
        for s, to in enumerate(zpeers):
            moves.append((last_edge.at[rows], last_got.at[s, rows], {"gz": to}))
        return remote(moves, last_sem, (k,))

    def r_moves():
        moves = [
            (r_sent.at[0], r_got.at[1], {"gx": near["gx"][0]}),
            (r_sent.at[1], r_got.at[0], {"gx": near["gx"][1]}),
            (r_sent.at[2], r_got.at[3], {"gy": near["gy"][0]}),
            (r_sent.at[3], r_got.at[2], {"gy": near["gy"][1]}),
        ]
        for s, to in enumerate(zpeers):
            moves.append((r_sent.at[4], r_got.at[4 + s], {"gz": to}))
        return remote(moves, r_sem, ())

    def one_moves(k):
        return deep_moves(one_a, one_edge, one_got, one_sem, k)

    def two_moves(k):
        return deep_moves(two_a, two_edge, two_got, two_sem, k)

    def go(moves):
        for copy in moves:
            copy.start()

    def arrive(moves):
        for copy in moves:
            copy.wait_recv()

    def leave(moves):
        for copy in moves:
            copy.wait_send()

    def roll(v, shift):
        return pltpu.roll(v, shift % nz, v.ndim - 1)

    def pack(get, ax, ay, w):
        acc = jnp.zeros((8, nz), jnp.float32)
        for x in range(ax):
            for y in range(ay):
                at = 2 * w * (x * ay + y)
                here = (lane >= at) & (lane < at + 2 * w)
                acc = jnp.where(here, roll(get(x, y), at + w), acc)
        return acc

    def edge_at(got, spot, w):
        return roll(got, -(2 * w * spot) - w)

    def join(got, w):
        if sides == 1:
            return got(0)
        return jnp.where((lane & (2 * w - 1)) < w, got(0), got(1))

    def along_z(v, h, w):
        low = roll(jnp.where(lane >= nz - w, h, v), w)
        high = roll(jnp.where(lane < w, h, v), -w)
        return low + high

    def pair_sum(v, w):
        even = (lane & (2 * w - 1)) < w
        return v + jnp.where(even, roll(v, -w), roll(v, w))

    def sweep_edges(own, ends, r, ax, ay, w, coupling):
        cell = w // 2
        mid, xm, xp, ym, yp = ends
        sy, sx = 2 * w, 2 * w * ay
        spot = lane // sy
        yi, xi = spot % ay, spot // ay
        z = jnp.where(
            (lane & (2 * w - 1)) >= w,
            roll(mid, -cell) + roll(own, cell),
            roll(mid, cell) + roll(own, -cell),
        )
        total = z + jnp.where(yi == ay - 1, roll(yp, sy * (ay - 1)), roll(mid, -sy))
        total = total + jnp.where(yi == 0, roll(ym, -sy * (ay - 1)), roll(mid, sy))
        total = total + jnp.where(xi == ax - 1, roll(xp, sx * (ax - 1)), roll(mid, -sx))
        total = total + jnp.where(xi == 0, roll(xm, -sx * (ax - 1)), roll(mid, sx))
        return (2.0 - jacobi_weight) * mid + coupling * r * total

    def sweep_wide(src, dst, ends, r_at, rows, ax, ay, w, coupling):
        mid, xm, xp, ym, yp = ends
        cells = [(x, y, mid, x * ay + y) for x in range(ax) for y in range(ay)]
        cells += [(-1, y, xm, (ax - 1) * ay + y) for y in range(ay)]
        cells += [(ax, y, xp, y) for y in range(ay)]
        cells += [(x, -1, ym, x * ay + ay - 1) for x in range(ax)]
        cells += [(x, ay, yp, x * ay) for x in range(ax)]
        for x, y, got, spot in cells:
            c = src[x + 2, y + 2, rows]
            total = (src[x + 1, y + 2, rows] + src[x + 3, y + 2, rows]) + (
                src[x + 2, y + 1, rows] + src[x + 2, y + 3, rows]
            )
            total = total + along_z(c, edge_at(got, spot, w), w // 2)
            dst[x + 1, y + 1, rows] = (2.0 - jacobi_weight) * c + coupling * r_at(x, y) * total

    def total_of(e, x, y, rows, h, w):
        c = e[x + 1, y + 1, rows]
        total = (e[x, y + 1, rows] + e[x + 2, y + 1, rows]) + (
            e[x + 1, y, rows] + e[x + 1, y + 2, rows]
        )
        return c, total + along_z(c, h, w)

    def around(p, sl, got, x):
        e = fine[p]
        c = e[x + 1, pl.ds(1, ny), sl]
        total = e[x, pl.ds(1, ny), sl] + e[x + 2, pl.ds(1, ny), sl]
        total = total + (e[x + 1, pl.ds(0, ny), sl] + e[x + 1, pl.ds(2, ny), sl])
        h = jnp.stack([edge_at(got, x * ny + y, 1) for y in range(ny)])
        low = roll(jnp.where(lane[None] >= nz - 1, h, c), 1)
        high = roll(jnp.where(lane[None] < 1, h, c), -1)
        return c, total + (low + high)

    def fine_edges(p, sl):
        return join(lambda s: zrecv[p, s, sl], 1)

    def fine_pack(p, sl):
        zsend[p, sl] = pack(lambda x, y: fine[p][x + 1, y + 1, sl], nx, ny, 1)

    def slab(k, i):
        return pl.ds(pl.multiple_of(k * width + i * 8, 8), 8)

    for small in smalls:
        small.wait()
    for g in range(bands // 8):
        m = jnp.zeros((8, nz), jnp.float32)
        s = jnp.ones((8, nz), jnp.float32)
        for j in range(8):
            m = jnp.where(sub == j, centre[g * 8 + j], m)
            s = jnp.where(sub == j, half_width[g * 8 + j], s)
        band_a[pl.ds(g * 8, 8)] = 3.0 - m
        band_i[pl.ds(g * 8, 8)] = 1.0 / s
    for x in range(nx):
        for y in range(ny):
            pot_b[x, y] = jnp.broadcast_to(pot[x, pl.ds(y, 1), :], (8, nz))
    for x2 in range(qx):
        for y2 in range(qy):
            quad = jnp.zeros((8, nz), jnp.float32)
            for hx in range(2):
                for hy in range(2):
                    x, y = 2 * x2 + hx, 2 * y2 + hy
                    v = pot_b[2 * x, 2 * y] + pot_b[2 * x + 1, 2 * y]
                    v = v + (pot_b[2 * x, 2 * y + 1] + pot_b[2 * x + 1, 2 * y + 1])
                    one = 0.125 * pair_sum(v, 1)
                    quad = quad + one
                    d1 = 0.75 + one + shift_mass
                    d1_b[x, y] = d1
                    r1_b[x + 1, y + 1] = jacobi_weight / d1
            r2_b[x2 + 1, y2 + 1] = jacobi_weight / (0.1875 + 0.125 * pair_sum(quad, 2) + shift_mass)
    for j, (x, y) in enumerate([(0, None), (mx - 1, None), (None, 0), (None, my - 1)]):
        for i in range(my if y is None else mx):
            cx, cy = (x, i) if y is None else (i, y)
            r_sent[j, pl.ds(i, 1)] = r1_b[cx + 1, cy + 1][0:1]
    for j, (x, y) in enumerate([(0, None), (qx - 1, None), (None, 0), (None, qy - 1)]):
        base = my if y is None else mx
        for i in range(qy if y is None else qx):
            cx, cy = (x, i) if y is None else (i, y)
            r_sent[j, pl.ds(base + i, 1)] = r2_b[cx + 1, cy + 1][0:1]
    r_sent[4, pl.ds(0, 1)] = pack(lambda x, y: r1_b[x + 1, y + 1], mx, my, 4)[0:1]
    r_sent[4, pl.ds(1, 1)] = pack(lambda x, y: r2_b[x + 1, y + 1], qx, qy, 8)[0:1]

    def ready(k, carry):
        rows = pl.ds(pl.multiple_of(k * width, 8), width)
        whole = fine[ORB].at[pl.ds(1, nx), pl.ds(1, ny), rows]
        pltpu.make_async_copy(whole, whole, load_sem.at[k]).wait()

        def inner(i, c):
            fine_pack(ORB, slab(k, i))
            return c

        lax.fori_loop(0, groups, inner, 0)
        return carry

    lax.fori_loop(0, chunks, ready, 0)

    pl.semaphore_wait(barrier, len(peers))
    lax.fori_loop(0, chunks, lambda k, c: (go(fine_moves(ORB, k)), c)[1], 0)
    go(r_moves())

    def step_first(k, carry):
        arrive(fine_moves(ORB, k))

        def inner(i, c):
            sl = slab(k, i)
            got = fine_edges(ORB, sl)
            a, f = band_a[sl], band_i[sl]
            for x in range(nx):
                v, total = around(ORB, sl, got, x)
                fine[FIRST][x + 1, pl.ds(1, ny), sl] = ((pot_b[x] + a) * v - 0.5 * total) * f
            fine_pack(FIRST, sl)
            return c

        lax.fori_loop(0, groups, inner, 0)
        go(fine_moves(FIRST, k))
        return carry

    lax.fori_loop(0, chunks, step_first, 0)

    arrive(r_moves())
    for i in range(my):
        for j, x in ((0, 0), (1, mx + 1)):
            r1_b[x, i + 1] = jnp.broadcast_to(r_got[j, pl.ds(i, 1)], (8, nz))
    for i in range(mx):
        for j, y in ((2, 0), (3, my + 1)):
            r1_b[i + 1, y] = jnp.broadcast_to(r_got[j, pl.ds(i, 1)], (8, nz))
    for i in range(qy):
        for j, x in ((0, 0), (1, qx + 1)):
            r2_b[x, i + 1] = jnp.broadcast_to(r_got[j, pl.ds(my + i, 1)], (8, nz))
    for i in range(qx):
        for j, y in ((2, 0), (3, qy + 1)):
            r2_b[i + 1, y] = jnp.broadcast_to(r_got[j, pl.ds(mx + i, 1)], (8, nz))

    def r_edge(row, w):
        return join(lambda s: jnp.broadcast_to(r_got[4 + s, pl.ds(row, 1)], (8, nz)), w)

    def step_second(k, carry):
        arrive(fine_moves(FIRST, k))
        packed = pl.ds(pl.multiple_of(k * 8, 8), 8)

        def inner(i, c):
            sl = slab(k, i)
            mine = (lane & 1) == i
            got = fine_edges(FIRST, sl)
            a, f = band_a[sl], 2.0 * band_i[sl]
            for x2 in range(mx):
                both = None
                for x in (2 * x2, 2 * x2 + 1):
                    v, total = around(FIRST, sl, got, x)
                    v = ((pot_b[x] + a) * v - 0.5 * total) * f - fine[ORB][x + 1, pl.ds(1, ny), sl]
                    second[x, :, sl] = v
                    both = v if both is None else both + v
                for y2 in range(my):
                    s = 0.5 * pair_sum(both[2 * y2] + both[2 * y2 + 1], 1)
                    one_a[x2 + 2, y2 + 2, packed] = jnp.where(
                        mine, r1_b[x2 + 1, y2 + 1] * s, one_a[x2 + 2, y2 + 2, packed]
                    )
            return c

        lax.fori_loop(0, groups, inner, 0)
        one_edge[packed] = pack(lambda x, y: one_a[x + 2, y + 2, packed], mx, my, 4)
        go(one_moves(k))
        return carry

    lax.fori_loop(0, chunks, step_second, 0)

    def step_residue(k, carry):
        arrive(one_moves(k))
        packed = pl.ds(pl.multiple_of(k * 8, 8), 8)
        rows = pl.ds(pl.multiple_of(lax.div(k, 2) * 8, 8), 8)
        mine = ((lane >> 1) & 1) == lax.rem(k, 2)
        ends = [join(lambda s, j=j: one_got[s, j, packed], 4) for j in range(5)]
        halo = sweep_edges(one_edge[packed], ends, r_edge(0, 4), mx, my, 4, 0.125)
        one_halo[packed] = halo
        sweep_wide(
            one_a, one_b, ends, lambda x, y: r1_b[x + 1, y + 1], packed, mx, my, 4, 0.125
        )
        for x2 in range(qx):
            for y2 in range(qy):
                acc = None
                for x in (2 * x2, 2 * x2 + 1):
                    for y in (2 * y2, 2 * y2 + 1):
                        h = edge_at(halo, x * my + y, 4)
                        c, total = total_of(one_b, x, y, packed, h, 2)
                        d = d1_b[x, y]
                        source = one_a[x + 2, y + 2, packed] * (d * (1.0 / jacobi_weight))
                        v = source - d * c + 0.125 * total
                        acc = v if acc is None else acc + v
                s = 0.5 * pair_sum(acc, 2)
                two_a[x2 + 2, y2 + 2, rows] = jnp.where(
                    mine, r2_b[x2 + 1, y2 + 1] * s, two_a[x2 + 2, y2 + 2, rows]
                )
        return carry

    def pair_residue(k, carry):
        lax.fori_loop(2 * k, 2 * k + 2, step_residue, 0)
        rows = pl.ds(pl.multiple_of(k * 8, 8), 8)
        two_edge[rows] = pack(lambda x, y: two_a[x + 2, y + 2, rows], qx, qy, 8)
        go(two_moves(k))
        return carry

    lax.fori_loop(0, pairs, pair_residue, 0)

    def step_two(k, carry):
        arrive(two_moves(k))
        rows = pl.ds(pl.multiple_of(k * 8, 8), 8)
        ends = [join(lambda s, j=j: two_got[s, j, rows], 8) for j in range(5)]
        halo = sweep_edges(two_edge[rows], ends, r_edge(1, 8), qx, qy, 8, 0.03125)
        sweep_wide(
            two_a, two_b, ends, lambda x, y: r2_b[x + 1, y + 1], rows, qx, qy, 8, 0.03125
        )
        for x in range(qx):
            for y in range(qy):
                c, total = total_of(two_b, x, y, rows, edge_at(halo, x * qy + y, 8), 4)
                two_c[x + 1, y + 1, rows] = (
                    (1.0 - jacobi_weight) * c
                    + two_a[x + 2, y + 2, rows]
                    + 0.03125 * r2_b[x + 1, y + 1] * total
                )
        last_edge[rows] = pack(lambda x, y: two_c[x + 1, y + 1, rows], qx, qy, 4)
        go(last_moves(k))
        return carry

    lax.fori_loop(0, pairs, step_two, 0)

    def step_last(k, half):
        rows = pl.ds(pl.multiple_of(k * 8, 8), 8)
        packed = pl.ds(pl.multiple_of(k * 16 + half * 8, 8), 8)
        left = (lane & 2) == 0

        def spread(v):
            return jnp.where(left, v, roll(v, 2)) if half == 0 else jnp.where(left, roll(v, -2), v)

        coarse = {}
        for x in range(-1, qx + 1):
            for y in range(-1, qy + 1):
                if 0 <= x < qx or 0 <= y < qy:
                    coarse[x, y] = spread(two_c[x + 1, y + 1, rows])
        got = join(lambda s: last_got[s, rows], 4)
        ends = {
            (x, y): spread(edge_at(got, x * qy + y, 4)) for x in range(qx) for y in range(qy)
        }
        halo = one_halo[packed]

        def at(x, y):
            return one_b[x + 1, y + 1, packed] + coarse[(x + 2) // 2 - 1, (y + 2) // 2 - 1]

        for x in range(mx):
            for y in range(my):
                c = at(x, y)
                total = (at(x - 1, y) + at(x + 1, y)) + (at(x, y - 1) + at(x, y + 1))
                h = edge_at(halo, x * my + y, 4) + ends[x // 2, y // 2]
                total = total + along_z(c, h, 2)
                v = (1.0 - jacobi_weight) * c + one_a[x + 2, y + 2, packed]
                v = v + 0.125 * r1_b[x + 1, y + 1] * total
                odd = (lane & 1) == 1
                for i, w in enumerate((jnp.where(odd, roll(v, 1), v), jnp.where(odd, v, roll(v, -1)))):
                    sl = slab(2 * k + half, i)
                    for hx in range(2):
                        for hy in range(2):
                            fx, fy = 2 * x + hx, 2 * y + hy
                            second[fx, fy, sl] = second[fx, fy, sl] + w

    def finish(k, carry):
        arrive(last_moves(k))
        for half in range(2):
            step_last(k, half)
            rows = pl.ds(pl.multiple_of((2 * k + half) * width, 8), width)

            def line(x, c):
                for y in range(ny):
                    pltpu.make_async_copy(
                        second.at[x, y, rows], out.at[rows, x, y], store_sem.at[2 * k + half]
                    ).start()
                return c

            lax.fori_loop(0, nx, line, 0)
        return carry

    lax.fori_loop(0, pairs, finish, 0)

    def drain(k, carry):
        rows = pl.ds(pl.multiple_of(k * width, 8), width)
        for p in (ORB, FIRST):
            leave(fine_moves(p, k))
        leave(one_moves(k))
        whole = second.at[:, :, rows]
        pltpu.make_async_copy(whole, whole, store_sem.at[k]).wait()
        return carry

    lax.fori_loop(0, chunks, drain, 0)

    def drain_pair(k, carry):
        leave(two_moves(k))
        leave(last_moves(k))
        return carry

    lax.fori_loop(0, pairs, drain_pair, 0)
    leave(r_moves())


def local(sizes, chunks, orbitals, potential, centre, half_width):
    bands, nx, ny, nz = orbitals.shape
    sides = 2 if sizes["gz"] > 2 else 1
    pairs = chunks // 2

    def f32(*shape):
        return pltpu.VMEM(shape, jnp.float32)

    def padded(cut, halo):
        return f32(nx // cut + 2 * halo, ny // cut + 2 * halo, bands if cut == 1 else bands // cut, nz)

    dma = pltpu.SemaphoreType.DMA
    deep = 8 + 5 * sides
    scratch = [padded(1, 1)] * 2 + [padded(2, 2), padded(2, 1), padded(4, 2), padded(4, 1), padded(4, 1)]
    scratch += [
        f32(nx, ny, bands, nz),
        f32(2, bands, nz),
        f32(2, sides, bands, nz),
        f32(bands // 2, nz),
        f32(sides, 5, bands // 2, nz),
        f32(bands // 2, nz),
        f32(bands // 4, nz),
        f32(sides, 5, bands // 4, nz),
        f32(bands // 4, nz),
        f32(sides, bands // 4, nz),
        f32(bands, nz),
        f32(bands, nz),
        f32(nx, ny, 8, nz),
        f32(nx // 2, ny // 2, 8, nz),
        f32(nx // 2 + 2, ny // 2 + 2, 8, nz),
        f32(nx // 4 + 2, ny // 4 + 2, 8, nz),
        f32(5, 8, nz),
        f32(4 + sides, 8, nz),
        dma((chunks,)),
        dma((chunks,)),
        dma((2, 2, chunks, 4 + sides)),
        dma((2, chunks, deep)),
        dma((2, pairs, deep)),
        dma((2, pairs, 4 + sides)),
        dma((2, 4 + sides)),
        pltpu.SMEM((bands,), jnp.float32),
        pltpu.SMEM((bands,), jnp.float32),
        f32(nx, ny, nz),
        dma((3,)),
    ]
    return pl.pallas_call(
        functools.partial(kernel, sizes, chunks),
        out_shape=jax.ShapeDtypeStruct(orbitals.shape, jnp.float32),
        in_specs=[pl.BlockSpec(memory_space=pltpu.HBM)] * 4,
        out_specs=pl.BlockSpec(memory_space=pl.ANY),
        scratch_shapes=scratch,
        compiler_params=pltpu.CompilerParams(
            collective_id=0, has_side_effects=True, vmem_limit_bytes=48 * 1024 * 1024
        ),
    )(*(pltpu.with_memory_space_constraint(v, pltpu.HBM) for v in (centre, half_width, potential, orbitals)))


def solution(mesh):
    in_specs = (P(None, "gx", "gy", "gz"), P("gx", "gy", "gz"), P(), P())
    out_specs = P(None, "gx", "gy", "gz")
    body = functools.partial(local, dict(mesh.shape), 4)
    return jax.shard_map(body, mesh=mesh, in_specs=in_specs, out_specs=out_specs, check_vma=False)
```

```python
import functools
import math

import jax
import jax.numpy as jnp
from jax import lax
from jax.experimental import pallas as pl
from jax.experimental.pallas import tpu as pltpu
from jax.sharding import PartitionSpec as P

shift_mass = 0.05
jacobi_weight = 2.0 / 3.0
MESH = pl.DeviceIdType.MESH
ORB, FIRST = range(2)


def kernel(sizes, chunks, centre_in, half_width_in, pot_in, orbitals, second, *scratch):
    fine = scratch[0:2]
    one_a, one_b, two_a, two_b, two_c = scratch[2:7]
    zsend, zrecv = scratch[7:9]
    one_edge, one_got, one_halo, two_edge, two_got, last_edge, last_got = scratch[9:16]
    band_a, band_i, pot_b, d1_b, r1_b, r2_b, r_sent, r_got = scratch[16:24]
    load_sem, send_sem, recv_sem, tally = scratch[24:28]
    centre, half_width, pot, small_sem = scratch[28:32]
    bands, nx, ny, nz = second.shape[2], second.shape[0], second.shape[1], second.shape[3]
    width = bands // chunks
    groups = width // 8
    pairs = chunks // 2
    mx, my, qx, qy = nx // 2, ny // 2, nx // 4, ny // 4
    sides = 2 if sizes["gz"] > 2 else 1
    at_one, at_two = 2 * chunks, 3 * chunks
    at_last, at_r = at_two + pairs, at_two + 2 * pairs
    lane = lax.broadcasted_iota(jnp.int32, (8, nz), 1)
    sub = lax.broadcasted_iota(jnp.int32, (8, nz), 0)

    near = {}
    for axis in ("gx", "gy", "gz"):
        me, n = lax.axis_index(axis), sizes[axis]
        near[axis] = (lax.rem(me + n - 1, n), lax.rem(me + 1, n))
    zpeers = [near["gz"][1], near["gz"][0]][:sides]
    peers = [{"gx": v} for v in near["gx"]] + [{"gy": v} for v in near["gy"]]
    peers += [{"gz": v} for v in zpeers]

    barrier = pltpu.get_barrier_semaphore()
    for peer in peers:
        pl.semaphore_signal(barrier, inc=1, device_id=peer, device_id_type=MESH)

    smalls = [
        pltpu.make_async_copy(src, dst, small_sem.at[j])
        for j, (src, dst) in enumerate(
            [(centre_in, centre), (half_width_in, half_width), (pot_in, pot)]
        )
    ]
    for small in smalls:
        small.start()

    def loads(k):
        rows = pl.ds(pl.multiple_of(k * width, 8), width)

        def line(x, _):
            for y in range(ny):
                pltpu.make_async_copy(
                    orbitals.at[rows, x, y], fine[ORB].at[x + 1, y + 1, rows], load_sem.at[k]
                ).start()
            return 0

        lax.fori_loop(0, nx, line, 0)

    lax.fori_loop(0, chunks, lambda k, c: (loads(k), c)[1], 0)

    def tiles(moves):
        return sum(math.prod(src.shape) for src, _, _ in moves) // (8 * nz)

    def take(n, sem):
        whole = tally.at[pl.ds(0, n)]
        pltpu.make_async_copy(whole, whole, sem).wait()

    def go(moves, sent, got):
        for src, dst, to in moves:
            pltpu.make_async_remote_copy(
                src_ref=src,
                dst_ref=dst,
                send_sem=send_sem.at[sent],
                recv_sem=recv_sem.at[got],
                device_id=to,
                device_id_type=MESH,
            ).start()

    def arrive(moves, got):
        take(tiles(moves), recv_sem.at[got])

    def leave(moves, times, sent):
        take(times * tiles(moves), send_sem.at[sent])

    def fine_moves(p, k):
        e = fine[p]
        rows = pl.ds(pl.multiple_of(k * width, 8), width)
        ys, xs = pl.ds(1, ny), pl.ds(1, nx)
        moves = [
            (e.at[xs, 1, rows], e.at[xs, ny + 1, rows], {"gy": near["gy"][0]}),
            (e.at[xs, ny, rows], e.at[xs, 0, rows], {"gy": near["gy"][1]}),
            (e.at[1, ys, rows], e.at[nx + 1, ys, rows], {"gx": near["gx"][0]}),
            (e.at[nx, ys, rows], e.at[0, ys, rows], {"gx": near["gx"][1]}),
        ]
        for s, to in enumerate(zpeers):
            moves.append((zsend.at[p, rows], zrecv.at[p, s, rows], {"gz": to}))
        return moves

    def deep_moves(e, edge, got, k):
        ax, ay = e.shape[0] - 4, e.shape[1] - 4
        rows = pl.ds(pl.multiple_of(k * 8, 8), 8)
        ys, xs = pl.ds(2, ay), pl.ds(2, ax)
        lo, hix, hiy, topx, topy = pl.ds(0, 2), pl.ds(ax, 2), pl.ds(ay, 2), pl.ds(ax + 2, 2), pl.ds(ay + 2, 2)
        two = pl.ds(2, 2)
        (xm, xp), (ym, yp) = near["gx"], near["gy"]
        moves = [
            (e.at[xs, two, rows], e.at[xs, topy, rows], {"gy": ym}),
            (e.at[xs, hiy, rows], e.at[xs, lo, rows], {"gy": yp}),
            (e.at[two, ys, rows], e.at[topx, ys, rows], {"gx": xm}),
            (e.at[hix, ys, rows], e.at[lo, ys, rows], {"gx": xp}),
            (e.at[2, 2, rows], e.at[ax + 2, ay + 2, rows], {"gx": xm, "gy": ym}),
            (e.at[ax + 1, 2, rows], e.at[1, ay + 2, rows], {"gx": xp, "gy": ym}),
            (e.at[2, ay + 1, rows], e.at[ax + 2, 1, rows], {"gx": xm, "gy": yp}),
            (e.at[ax + 1, ay + 1, rows], e.at[1, 1, rows], {"gx": xp, "gy": yp}),
        ]
        for s, z in enumerate(zpeers):
            for j, to in enumerate([{}, {"gx": xp}, {"gx": xm}, {"gy": yp}, {"gy": ym}]):
                moves.append((edge.at[rows], got.at[s, j, rows], {"gz": z, **to}))
        return moves

    def last_moves(k):
        e = two_c
        rows = pl.ds(pl.multiple_of(k * 8, 8), 8)
        ys, xs = pl.ds(1, qy), pl.ds(1, qx)
        moves = [
            (e.at[xs, 1, rows], e.at[xs, qy + 1, rows], {"gy": near["gy"][0]}),
            (e.at[xs, qy, rows], e.at[xs, 0, rows], {"gy": near["gy"][1]}),
            (e.at[1, ys, rows], e.at[qx + 1, ys, rows], {"gx": near["gx"][0]}),
            (e.at[qx, ys, rows], e.at[0, ys, rows], {"gx": near["gx"][1]}),
        ]
        for s, to in enumerate(zpeers):
            moves.append((last_edge.at[rows], last_got.at[s, rows], {"gz": to}))
        return moves

    def r_moves():
        moves = [
            (r_sent.at[0], r_got.at[1], {"gx": near["gx"][0]}),
            (r_sent.at[1], r_got.at[0], {"gx": near["gx"][1]}),
            (r_sent.at[2], r_got.at[3], {"gy": near["gy"][0]}),
            (r_sent.at[3], r_got.at[2], {"gy": near["gy"][1]}),
        ]
        for s, to in enumerate(zpeers):
            moves.append((r_sent.at[4], r_got.at[4 + s], {"gz": to}))
        return moves

    def one_moves(k):
        return deep_moves(one_a, one_edge, one_got, k)

    def two_moves(k):
        return deep_moves(two_a, two_edge, two_got, k)

    def roll(v, shift):
        return pltpu.roll(v, shift % nz, v.ndim - 1)

    def pack(get, ax, ay, w):
        acc = jnp.zeros((8, nz), jnp.float32)
        for x in range(ax):
            for y in range(ay):
                at = 2 * w * (x * ay + y)
                here = (lane >= at) & (lane < at + 2 * w)
                acc = jnp.where(here, roll(get(x, y), at + w), acc)
        return acc

    def edge_at(got, spot, w):
        return roll(got, -(2 * w * spot) - w)

    def join(got, w):
        if sides == 1:
            return got(0)
        return jnp.where((lane & (2 * w - 1)) < w, got(0), got(1))

    def along_z(v, h, w):
        low = roll(jnp.where(lane >= nz - w, h, v), w)
        high = roll(jnp.where(lane < w, h, v), -w)
        return low + high

    def pair_sum(v, w):
        even = (lane & (2 * w - 1)) < w
        return v + jnp.where(even, roll(v, -w), roll(v, w))

    def sweep_edges(own, ends, r, ax, ay, w, coupling):
        cell = w // 2
        mid, xm, xp, ym, yp = ends
        sy, sx = 2 * w, 2 * w * ay
        spot = lane // sy
        yi, xi = spot % ay, spot // ay
        z = jnp.where(
            (lane & (2 * w - 1)) >= w,
            roll(mid, -cell) + roll(own, cell),
            roll(mid, cell) + roll(own, -cell),
        )
        total = z + jnp.where(yi == ay - 1, roll(yp, sy * (ay - 1)), roll(mid, -sy))
        total = total + jnp.where(yi == 0, roll(ym, -sy * (ay - 1)), roll(mid, sy))
        total = total + jnp.where(xi == ax - 1, roll(xp, sx * (ax - 1)), roll(mid, -sx))
        total = total + jnp.where(xi == 0, roll(xm, -sx * (ax - 1)), roll(mid, sx))
        return (2.0 - jacobi_weight) * mid + coupling * r * total

    def sweep_wide(src, dst, ends, r_at, rows, ax, ay, w, coupling):
        mid, xm, xp, ym, yp = ends
        cells = [(x, y, mid, x * ay + y) for x in range(ax) for y in range(ay)]
        cells += [(-1, y, xm, (ax - 1) * ay + y) for y in range(ay)]
        cells += [(ax, y, xp, y) for y in range(ay)]
        cells += [(x, -1, ym, x * ay + ay - 1) for x in range(ax)]
        cells += [(x, ay, yp, x * ay) for x in range(ax)]
        for x, y, got, spot in cells:
            c = src[x + 2, y + 2, rows]
            total = (src[x + 1, y + 2, rows] + src[x + 3, y + 2, rows]) + (
                src[x + 2, y + 1, rows] + src[x + 2, y + 3, rows]
            )
            total = total + along_z(c, edge_at(got, spot, w), w // 2)
            dst[x + 1, y + 1, rows] = (2.0 - jacobi_weight) * c + coupling * r_at(x, y) * total

    def total_of(e, x, y, rows, h, w):
        c = e[x + 1, y + 1, rows]
        total = (e[x, y + 1, rows] + e[x + 2, y + 1, rows]) + (
            e[x + 1, y, rows] + e[x + 1, y + 2, rows]
        )
        return c, total + along_z(c, h, w)

    def around(p, sl, got, x):
        e = fine[p]
        c = e[x + 1, pl.ds(1, ny), sl]
        total = e[x, pl.ds(1, ny), sl] + e[x + 2, pl.ds(1, ny), sl]
        total = total + (e[x + 1, pl.ds(0, ny), sl] + e[x + 1, pl.ds(2, ny), sl])
        h = jnp.stack([edge_at(got, x * ny + y, 1) for y in range(ny)])
        low = roll(jnp.where(lane[None] >= nz - 1, h, c), 1)
        high = roll(jnp.where(lane[None] < 1, h, c), -1)
        return c, total + (low + high)

    def fine_edges(p, sl):
        return join(lambda s: zrecv[p, s, sl], 1)

    def fine_pack(p, sl):
        zsend[p, sl] = pack(lambda x, y: fine[p][x + 1, y + 1, sl], nx, ny, 1)

    def slab(k, i):
        return pl.ds(pl.multiple_of(k * width + i * 8, 8), 8)

    def ready(k, carry):
        rows = pl.ds(pl.multiple_of(k * width, 8), width)
        whole = fine[ORB].at[pl.ds(1, nx), pl.ds(1, ny), rows]
        pltpu.make_async_copy(whole, whole, load_sem.at[k]).wait()
        return carry

    lax.fori_loop(0, chunks, ready, 0)
    pl.semaphore_wait(barrier, len(peers))
    lax.fori_loop(0, chunks, lambda k, c: (go(fine_moves(ORB, k)[:4], 0, k), c)[1], 0)

    def start_z(k, carry):
        def inner(i, c):
            fine_pack(ORB, slab(k, i))
            return c

        lax.fori_loop(0, groups, inner, 0)
        go(fine_moves(ORB, k)[4:], 0, k)
        return carry

    lax.fori_loop(0, chunks, start_z, 0)

    for small in smalls:
        small.wait()
    for g in range(bands // 8):
        m = jnp.zeros((8, nz), jnp.float32)
        s = jnp.ones((8, nz), jnp.float32)
        for j in range(8):
            m = jnp.where(sub == j, centre[g * 8 + j], m)
            s = jnp.where(sub == j, half_width[g * 8 + j], s)
        band_a[pl.ds(g * 8, 8)] = 3.0 - m
        band_i[pl.ds(g * 8, 8)] = 1.0 / s
    for x in range(nx):
        for y in range(ny):
            pot_b[x, y] = jnp.broadcast_to(pot[x, pl.ds(y, 1), :], (8, nz))
    for x2 in range(qx):
        for y2 in range(qy):
            quad = jnp.zeros((8, nz), jnp.float32)
            for hx in range(2):
                for hy in range(2):
                    x, y = 2 * x2 + hx, 2 * y2 + hy
                    v = pot_b[2 * x, 2 * y] + pot_b[2 * x + 1, 2 * y]
                    v = v + (pot_b[2 * x, 2 * y + 1] + pot_b[2 * x + 1, 2 * y + 1])
                    one = 0.125 * pair_sum(v, 1)
                    quad = quad + one
                    d1 = 0.75 + one + shift_mass
                    d1_b[x, y] = d1
                    r1_b[x + 1, y + 1] = jacobi_weight / d1
            r2_b[x2 + 1, y2 + 1] = jacobi_weight / (0.1875 + 0.125 * pair_sum(quad, 2) + shift_mass)
    for j, (x, y) in enumerate([(0, None), (mx - 1, None), (None, 0), (None, my - 1)]):
        for i in range(my if y is None else mx):
            cx, cy = (x, i) if y is None else (i, y)
            r_sent[j, pl.ds(i, 1)] = r1_b[cx + 1, cy + 1][0:1]
    for j, (x, y) in enumerate([(0, None), (qx - 1, None), (None, 0), (None, qy - 1)]):
        base = my if y is None else mx
        for i in range(qy if y is None else qx):
            cx, cy = (x, i) if y is None else (i, y)
            r_sent[j, pl.ds(base + i, 1)] = r2_b[cx + 1, cy + 1][0:1]
    r_sent[4, pl.ds(0, 1)] = pack(lambda x, y: r1_b[x + 1, y + 1], mx, my, 4)[0:1]
    r_sent[4, pl.ds(1, 1)] = pack(lambda x, y: r2_b[x + 1, y + 1], qx, qy, 8)[0:1]

    go(r_moves(), 5, at_r)

    def step_first(k, carry):
        arrive(fine_moves(ORB, k), k)

        def inner(i, c):
            sl = slab(k, i)
            got = fine_edges(ORB, sl)
            a, f = band_a[sl], band_i[sl]
            for x in range(nx):
                v, total = around(ORB, sl, got, x)
                fine[FIRST][x + 1, pl.ds(1, ny), sl] = ((pot_b[x] + a) * v - 0.5 * total) * f
            fine_pack(FIRST, sl)
            return c

        lax.fori_loop(0, groups, inner, 0)
        go(fine_moves(FIRST, k), 1, chunks + k)
        return carry

    lax.fori_loop(0, chunks, step_first, 0)

    arrive(r_moves(), at_r)
    for i in range(my):
        for j, x in ((0, 0), (1, mx + 1)):
            r1_b[x, i + 1] = jnp.broadcast_to(r_got[j, pl.ds(i, 1)], (8, nz))
    for i in range(mx):
        for j, y in ((2, 0), (3, my + 1)):
            r1_b[i + 1, y] = jnp.broadcast_to(r_got[j, pl.ds(i, 1)], (8, nz))
    for i in range(qy):
        for j, x in ((0, 0), (1, qx + 1)):
            r2_b[x, i + 1] = jnp.broadcast_to(r_got[j, pl.ds(my + i, 1)], (8, nz))
    for i in range(qx):
        for j, y in ((2, 0), (3, qy + 1)):
            r2_b[i + 1, y] = jnp.broadcast_to(r_got[j, pl.ds(mx + i, 1)], (8, nz))

    def r_edge(row, w):
        return join(lambda s: jnp.broadcast_to(r_got[4 + s, pl.ds(row, 1)], (8, nz)), w)

    def step_second(k, carry):
        arrive(fine_moves(FIRST, k), chunks + k)
        packed = pl.ds(pl.multiple_of(k * 8, 8), 8)

        def inner(i, c):
            sl = slab(k, i)
            mine = (lane & 1) == i
            got = fine_edges(FIRST, sl)
            a, f = band_a[sl], 2.0 * band_i[sl]
            for x2 in range(mx):
                both = None
                for x in (2 * x2, 2 * x2 + 1):
                    v, total = around(FIRST, sl, got, x)
                    v = ((pot_b[x] + a) * v - 0.5 * total) * f - fine[ORB][x + 1, pl.ds(1, ny), sl]
                    second[x, :, sl] = v
                    both = v if both is None else both + v
                for y2 in range(my):
                    s = 0.5 * pair_sum(both[2 * y2] + both[2 * y2 + 1], 1)
                    one_a[x2 + 2, y2 + 2, packed] = jnp.where(
                        mine, r1_b[x2 + 1, y2 + 1] * s, one_a[x2 + 2, y2 + 2, packed]
                    )
            return c

        lax.fori_loop(0, groups, inner, 0)
        one_edge[packed] = pack(lambda x, y: one_a[x + 2, y + 2, packed], mx, my, 4)
        go(one_moves(k), 2, at_one + k)
        return carry

    lax.fori_loop(0, chunks, step_second, 0)

    def step_residue(k, carry):
        arrive(one_moves(k), at_one + k)
        packed = pl.ds(pl.multiple_of(k * 8, 8), 8)
        rows = pl.ds(pl.multiple_of(lax.div(k, 2) * 8, 8), 8)
        mine = ((lane >> 1) & 1) == lax.rem(k, 2)
        ends = [join(lambda s, j=j: one_got[s, j, packed], 4) for j in range(5)]
        halo = sweep_edges(one_edge[packed], ends, r_edge(0, 4), mx, my, 4, 0.125)
        one_halo[packed] = halo
        sweep_wide(
            one_a, one_b, ends, lambda x, y: r1_b[x + 1, y + 1], packed, mx, my, 4, 0.125
        )
        for x2 in range(qx):
            for y2 in range(qy):
                acc = None
                for x in (2 * x2, 2 * x2 + 1):
                    for y in (2 * y2, 2 * y2 + 1):
                        h = edge_at(halo, x * my + y, 4)
                        c, total = total_of(one_b, x, y, packed, h, 2)
                        d = d1_b[x, y]
                        source = one_a[x + 2, y + 2, packed] * (d * (1.0 / jacobi_weight))
                        v = source - d * c + 0.125 * total
                        acc = v if acc is None else acc + v
                s = 0.5 * pair_sum(acc, 2)
                two_a[x2 + 2, y2 + 2, rows] = jnp.where(
                    mine, r2_b[x2 + 1, y2 + 1] * s, two_a[x2 + 2, y2 + 2, rows]
                )
        return carry

    def pair_residue(k, carry):
        lax.fori_loop(2 * k, 2 * k + 2, step_residue, 0)
        rows = pl.ds(pl.multiple_of(k * 8, 8), 8)
        two_edge[rows] = pack(lambda x, y: two_a[x + 2, y + 2, rows], qx, qy, 8)
        go(two_moves(k), 3, at_two + k)
        return carry

    lax.fori_loop(0, pairs, pair_residue, 0)

    def step_two(k, carry):
        arrive(two_moves(k), at_two + k)
        rows = pl.ds(pl.multiple_of(k * 8, 8), 8)
        ends = [join(lambda s, j=j: two_got[s, j, rows], 8) for j in range(5)]
        halo = sweep_edges(two_edge[rows], ends, r_edge(1, 8), qx, qy, 8, 0.03125)
        sweep_wide(
            two_a, two_b, ends, lambda x, y: r2_b[x + 1, y + 1], rows, qx, qy, 8, 0.03125
        )
        for x in range(qx):
            for y in range(qy):
                c, total = total_of(two_b, x, y, rows, edge_at(halo, x * qy + y, 8), 4)
                two_c[x + 1, y + 1, rows] = (
                    (1.0 - jacobi_weight) * c
                    + two_a[x + 2, y + 2, rows]
                    + 0.03125 * r2_b[x + 1, y + 1] * total
                )
        last_edge[rows] = pack(lambda x, y: two_c[x + 1, y + 1, rows], qx, qy, 4)
        go(last_moves(k), 4, at_last + k)
        return carry

    lax.fori_loop(0, pairs, step_two, 0)

    def step_last(k, half):
        rows = pl.ds(pl.multiple_of(k * 8, 8), 8)
        packed = pl.ds(pl.multiple_of(k * 16 + half * 8, 8), 8)
        left = (lane & 2) == 0

        def spread(v):
            return jnp.where(left, v, roll(v, 2)) if half == 0 else jnp.where(left, roll(v, -2), v)

        coarse = {}
        for x in range(-1, qx + 1):
            for y in range(-1, qy + 1):
                if 0 <= x < qx or 0 <= y < qy:
                    coarse[x, y] = spread(two_c[x + 1, y + 1, rows])
        got = join(lambda s: last_got[s, rows], 4)
        ends = {
            (x, y): spread(edge_at(got, x * qy + y, 4)) for x in range(qx) for y in range(qy)
        }
        halo = one_halo[packed]

        def at(x, y):
            return one_b[x + 1, y + 1, packed] + coarse[(x + 2) // 2 - 1, (y + 2) // 2 - 1]

        for x in range(mx):
            for y in range(my):
                c = at(x, y)
                total = (at(x - 1, y) + at(x + 1, y)) + (at(x, y - 1) + at(x, y + 1))
                h = edge_at(halo, x * my + y, 4) + ends[x // 2, y // 2]
                total = total + along_z(c, h, 2)
                v = (1.0 - jacobi_weight) * c + one_a[x + 2, y + 2, packed]
                v = v + 0.125 * r1_b[x + 1, y + 1] * total
                odd = (lane & 1) == 1
                for i, w in enumerate((jnp.where(odd, roll(v, 1), v), jnp.where(odd, v, roll(v, -1)))):
                    sl = slab(2 * k + half, i)
                    for hx in range(2):
                        for hy in range(2):
                            fx, fy = 2 * x + hx, 2 * y + hy
                            second[fx, fy, sl] = second[fx, fy, sl] + w

    def finish(k, carry):
        arrive(last_moves(k), at_last + k)
        for half in range(2):
            step_last(k, half)
        return carry

    lax.fori_loop(0, pairs, finish, 0)

    leave(fine_moves(ORB, 0), chunks, 0)
    leave(fine_moves(FIRST, 0), chunks, 1)
    leave(one_moves(0), chunks, 2)
    leave(two_moves(0), pairs, 3)
    leave(last_moves(0), pairs, 4)
    leave(r_moves(), 1, 5)


def store(filtered, out, sem):
    nx, ny = filtered.shape[:2]

    def line(x, c):
        for y in range(ny):
            pltpu.make_async_copy(filtered.at[x, y], out.at[:, x, y], sem).start()
        return c

    lax.fori_loop(0, nx, line, 0)
    pltpu.make_async_copy(filtered, filtered, sem).wait()


def local(sizes, chunks, orbitals, potential, centre, half_width):
    bands, nx, ny, nz = orbitals.shape
    sides = 2 if sizes["gz"] > 2 else 1
    pairs = chunks // 2

    def f32(*shape):
        return pltpu.VMEM(shape, jnp.float32)

    def padded(cut, halo):
        return f32(nx // cut + 2 * halo, ny // cut + 2 * halo, bands if cut == 1 else bands // cut, nz)

    dma = pltpu.SemaphoreType.DMA
    scratch = [padded(1, 1)] * 2 + [padded(2, 2), padded(2, 1), padded(4, 2), padded(4, 1), padded(4, 1)]
    scratch += [
        f32(2, bands, nz),
        f32(2, sides, bands, nz),
        f32(bands // 2, nz),
        f32(sides, 5, bands // 2, nz),
        f32(bands // 2, nz),
        f32(bands // 4, nz),
        f32(sides, 5, bands // 4, nz),
        f32(bands // 4, nz),
        f32(sides, bands // 4, nz),
        f32(bands, nz),
        f32(bands, nz),
        f32(nx, ny, 8, nz),
        f32(nx // 2, ny // 2, 8, nz),
        f32(nx // 2 + 2, ny // 2 + 2, 8, nz),
        f32(nx // 4 + 2, ny // 4 + 2, 8, nz),
        f32(5, 8, nz),
        f32(4 + sides, 8, nz),
        dma((chunks,)),
        dma((6,)),
        dma((3 * chunks + 2 * pairs + 1,)),
        f32((2 * (nx + ny) + sides) * bands // 8, 8, nz),
        pltpu.SMEM((bands,), jnp.float32),
        pltpu.SMEM((bands,), jnp.float32),
        f32(nx, ny, nz),
        dma((3,)),
    ]
    filtered = pl.pallas_call(
        functools.partial(kernel, sizes, chunks),
        out_shape=pltpu.VMEM((nx, ny, bands, nz), jnp.float32),
        in_specs=[pl.BlockSpec(memory_space=pltpu.HBM)] * 4,
        out_specs=pl.BlockSpec(memory_space=pltpu.VMEM),
        scratch_shapes=scratch,
        compiler_params=pltpu.CompilerParams(
            collective_id=0, has_side_effects=True, vmem_limit_bytes=48 * 1024 * 1024
        ),
    )(*(pltpu.with_memory_space_constraint(v, pltpu.HBM) for v in (centre, half_width, potential, orbitals)))
    return pl.pallas_call(
        store,
        out_shape=jax.ShapeDtypeStruct(orbitals.shape, jnp.float32),
        in_specs=[pl.BlockSpec(memory_space=pltpu.VMEM)],
        out_specs=pl.BlockSpec(memory_space=pltpu.HBM),
        scratch_shapes=[dma(())],
    )(pltpu.with_memory_space_constraint(filtered, pltpu.VMEM))


def solution(mesh):
    in_specs = (P(None, "gx", "gy", "gz"), P("gx", "gy", "gz"), P(), P())
    out_specs = P(None, "gx", "gy", "gz")
    body = functools.partial(local, dict(mesh.shape), 4)
    return jax.shard_map(body, mesh=mesh, in_specs=in_specs, out_specs=out_specs, check_vma=False)
```

```python
import functools
import math

import jax
import jax.numpy as jnp
from jax import lax
from jax.experimental import pallas as pl
from jax.experimental.pallas import tpu as pltpu
from jax.sharding import PartitionSpec as P

shift_mass = 0.05
jacobi_weight = 2.0 / 3.0
MESH = pl.DeviceIdType.MESH
ORB, FIRST = range(2)


def kernel(sizes, chunks, centre_in, half_width_in, pot_in, orbitals, second, *scratch):
    fine = scratch[0:2]
    one_a, one_b, two_a, two_b, two_c = scratch[2:7]
    zsend, zrecv = scratch[7:9]
    one_edge, one_got, one_halo, two_edge, two_got, last_edge, last_got = scratch[9:16]
    band_a, band_i, pot_b, d1_b, r1_b, r2_b, r_sent, r_got = scratch[16:24]
    load_sem, send_sem, recv_sem, tally = scratch[24:28]
    centre, half_width, pot, small_sem, token = scratch[28:33]
    bands, nx, ny, nz = second.shape[2], second.shape[0], second.shape[1], second.shape[3]
    width = bands // chunks
    groups = width // 8
    pairs = chunks // 2
    early = chunks // 2
    mx, my, qx, qy = nx // 2, ny // 2, nx // 4, ny // 4
    sides = 2 if sizes["gz"] > 2 else 1
    at_one, at_two = 2 * chunks, 3 * chunks
    at_last, at_r = at_two + pairs, at_two + 2 * pairs
    lane = lax.broadcasted_iota(jnp.int32, (8, nz), 1)
    sub = lax.broadcasted_iota(jnp.int32, (8, nz), 0)

    near = {}
    for axis in ("gx", "gy", "gz"):
        me, n = lax.axis_index(axis), sizes[axis]
        near[axis] = (lax.rem(me + n - 1, n), lax.rem(me + 1, n))
    zpeers = [near["gz"][1], near["gz"][0]][:sides]
    gy, ylast = lax.axis_index("gy"), sizes["gy"] - 1
    peers = [{"gx": v} for v in near["gx"]] + [{"gz": v} for v in zpeers]

    def signal(sem, to):
        pl.semaphore_signal(sem, inc=1, device_id=to, device_id_type=MESH)

    barrier = pltpu.get_barrier_semaphore()
    for peer in peers:
        signal(barrier, peer)

    @pl.when(gy > 0)
    def _():
        signal(barrier, {"gy": gy - 1})

    @pl.when(gy < ylast)
    def _():
        signal(barrier, {"gy": gy + 1})

    ycount = lax.div(gy + ylast, ylast + 1) + lax.div(2 * ylast - gy, ylast + 1)

    smalls = [
        pltpu.make_async_copy(src, dst, small_sem.at[j])
        for j, (src, dst) in enumerate(
            [(centre_in, centre), (half_width_in, half_width), (pot_in, pot)]
        )
    ]
    for small in smalls:
        small.start()

    def load(x, c):
        for y in range(ny):
            pltpu.make_async_copy(
                orbitals.at[:, x, y], fine[ORB].at[x + 1, y + 1], load_sem.at[0]
            ).start()
        return c

    lax.fori_loop(0, nx, load, 0)

    def tiles(moves):
        return sum(math.prod(src.shape) for src, _, _ in moves) // (8 * nz)

    def take(n, sem):
        whole = tally.at[pl.ds(0, n)]
        pltpu.make_async_copy(whole, whole, sem).wait()

    def go(moves, sent, got):
        for src, dst, to in moves:
            pltpu.make_async_remote_copy(
                src_ref=src,
                dst_ref=dst,
                send_sem=send_sem.at[sent],
                recv_sem=recv_sem.at[got],
                device_id=to,
                device_id_type=MESH,
            ).start()

    def go_split(downs, ups, rest, sent, got):
        @pl.when(gy == ylast)
        def _():
            go(ups + downs, sent, got)

        @pl.when(gy != ylast)
        def _():
            go(downs + ups, sent, got)

        go(rest, sent, got)

    def go_faces(moves, sent, got):
        go_split(moves[:1], moves[1:2], moves[2:], sent, got)

    def go_deep(moves, sent, got):
        downs, ups = [moves[0], *moves[4:6]], [moves[1], *moves[6:8]]
        rest = moves[2:4]
        for s in range(sides):
            ends = moves[8 + 5 * s : 13 + 5 * s]
            rest, ups, downs = rest + ends[:3], ups + ends[3:4], downs + ends[4:]
        go_split(downs, ups, rest, sent, got)

    def arrive(moves, got):
        take(tiles(moves), recv_sem.at[got])

    def leave(moves, times, sent):
        take(times * tiles(moves), send_sem.at[sent])

    def fine_moves(p, k):
        e = fine[p]
        rows = pl.ds(pl.multiple_of(k * width, 8), width)
        ys, xs = pl.ds(1, ny), pl.ds(1, nx)
        moves = [
            (e.at[xs, 1, rows], e.at[xs, ny + 1, rows], {"gy": near["gy"][0]}),
            (e.at[xs, ny, rows], e.at[xs, 0, rows], {"gy": near["gy"][1]}),
            (e.at[1, ys, rows], e.at[nx + 1, ys, rows], {"gx": near["gx"][0]}),
            (e.at[nx, ys, rows], e.at[0, ys, rows], {"gx": near["gx"][1]}),
        ]
        for s, to in enumerate(zpeers):
            moves.append((zsend.at[p, rows], zrecv.at[p, s, rows], {"gz": to}))
        return moves

    def deep_moves(e, edge, got, k):
        ax, ay = e.shape[0] - 4, e.shape[1] - 4
        rows = pl.ds(pl.multiple_of(k * 8, 8), 8)
        ys, xs = pl.ds(2, ay), pl.ds(2, ax)
        lo, hix, hiy, topx, topy = pl.ds(0, 2), pl.ds(ax, 2), pl.ds(ay, 2), pl.ds(ax + 2, 2), pl.ds(ay + 2, 2)
        two = pl.ds(2, 2)
        (xm, xp), (ym, yp) = near["gx"], near["gy"]
        moves = [
            (e.at[xs, two, rows], e.at[xs, topy, rows], {"gy": ym}),
            (e.at[xs, hiy, rows], e.at[xs, lo, rows], {"gy": yp}),
            (e.at[two, ys, rows], e.at[topx, ys, rows], {"gx": xm}),
            (e.at[hix, ys, rows], e.at[lo, ys, rows], {"gx": xp}),
            (e.at[2, 2, rows], e.at[ax + 2, ay + 2, rows], {"gx": xm, "gy": ym}),
            (e.at[ax + 1, 2, rows], e.at[1, ay + 2, rows], {"gx": xp, "gy": ym}),
            (e.at[2, ay + 1, rows], e.at[ax + 2, 1, rows], {"gx": xm, "gy": yp}),
            (e.at[ax + 1, ay + 1, rows], e.at[1, 1, rows], {"gx": xp, "gy": yp}),
        ]
        for s, z in enumerate(zpeers):
            for j, to in enumerate([{}, {"gx": xp}, {"gx": xm}, {"gy": yp}, {"gy": ym}]):
                moves.append((edge.at[rows], got.at[s, j, rows], {"gz": z, **to}))
        return moves

    def last_moves(k):
        e = two_c
        rows = pl.ds(pl.multiple_of(k * 8, 8), 8)
        ys, xs = pl.ds(1, qy), pl.ds(1, qx)
        moves = [
            (e.at[xs, 1, rows], e.at[xs, qy + 1, rows], {"gy": near["gy"][0]}),
            (e.at[xs, qy, rows], e.at[xs, 0, rows], {"gy": near["gy"][1]}),
            (e.at[1, ys, rows], e.at[qx + 1, ys, rows], {"gx": near["gx"][0]}),
            (e.at[qx, ys, rows], e.at[0, ys, rows], {"gx": near["gx"][1]}),
        ]
        for s, to in enumerate(zpeers):
            moves.append((last_edge.at[rows], last_got.at[s, rows], {"gz": to}))
        return moves

    def r_moves():
        moves = [
            (r_sent.at[0], r_got.at[1], {"gx": near["gx"][0]}),
            (r_sent.at[1], r_got.at[0], {"gx": near["gx"][1]}),
            (r_sent.at[2], r_got.at[3], {"gy": near["gy"][0]}),
            (r_sent.at[3], r_got.at[2], {"gy": near["gy"][1]}),
        ]
        for s, to in enumerate(zpeers):
            moves.append((r_sent.at[4], r_got.at[4 + s], {"gz": to}))
        return moves

    def one_moves(k):
        return deep_moves(one_a, one_edge, one_got, k)

    def two_moves(k):
        return deep_moves(two_a, two_edge, two_got, k)

    def roll(v, shift):
        return pltpu.roll(v, shift % nz, v.ndim - 1)

    def pack(get, ax, ay, w):
        acc = jnp.zeros((8, nz), jnp.float32)
        for x in range(ax):
            for y in range(ay):
                at = 2 * w * (x * ay + y)
                here = (lane >= at) & (lane < at + 2 * w)
                acc = jnp.where(here, roll(get(x, y), at + w), acc)
        return acc

    def edge_at(got, spot, w):
        return roll(got, -(2 * w * spot) - w)

    def join(got, w):
        if sides == 1:
            return got(0)
        return jnp.where((lane & (2 * w - 1)) < w, got(0), got(1))

    def along_z(v, h, w):
        low = roll(jnp.where(lane >= nz - w, h, v), w)
        high = roll(jnp.where(lane < w, h, v), -w)
        return low + high

    def pair_sum(v, w):
        even = (lane & (2 * w - 1)) < w
        return v + jnp.where(even, roll(v, -w), roll(v, w))

    def sweep_edges(own, ends, r, ax, ay, w, coupling):
        cell = w // 2
        mid, xm, xp, ym, yp = ends
        sy, sx = 2 * w, 2 * w * ay
        spot = lane // sy
        yi, xi = spot % ay, spot // ay
        z = jnp.where(
            (lane & (2 * w - 1)) >= w,
            roll(mid, -cell) + roll(own, cell),
            roll(mid, cell) + roll(own, -cell),
        )
        total = z + jnp.where(yi == ay - 1, roll(yp, sy * (ay - 1)), roll(mid, -sy))
        total = total + jnp.where(yi == 0, roll(ym, -sy * (ay - 1)), roll(mid, sy))
        total = total + jnp.where(xi == ax - 1, roll(xp, sx * (ax - 1)), roll(mid, -sx))
        total = total + jnp.where(xi == 0, roll(xm, -sx * (ax - 1)), roll(mid, sx))
        return (2.0 - jacobi_weight) * mid + coupling * r * total

    def sweep_wide(src, dst, ends, r_at, rows, ax, ay, w, coupling):
        mid, xm, xp, ym, yp = ends
        cells = [(x, y, mid, x * ay + y) for x in range(ax) for y in range(ay)]
        cells += [(-1, y, xm, (ax - 1) * ay + y) for y in range(ay)]
        cells += [(ax, y, xp, y) for y in range(ay)]
        cells += [(x, -1, ym, x * ay + ay - 1) for x in range(ax)]
        cells += [(x, ay, yp, x * ay) for x in range(ax)]
        for x, y, got, spot in cells:
            c = src[x + 2, y + 2, rows]
            total = (src[x + 1, y + 2, rows] + src[x + 3, y + 2, rows]) + (
                src[x + 2, y + 1, rows] + src[x + 2, y + 3, rows]
            )
            total = total + along_z(c, edge_at(got, spot, w), w // 2)
            dst[x + 1, y + 1, rows] = (2.0 - jacobi_weight) * c + coupling * r_at(x, y) * total

    def total_of(e, x, y, rows, h, w):
        c = e[x + 1, y + 1, rows]
        total = (e[x, y + 1, rows] + e[x + 2, y + 1, rows]) + (
            e[x + 1, y, rows] + e[x + 1, y + 2, rows]
        )
        return c, total + along_z(c, h, w)

    def around(p, sl, got, x):
        e = fine[p]
        c = e[x + 1, pl.ds(1, ny), sl]
        total = e[x, pl.ds(1, ny), sl] + e[x + 2, pl.ds(1, ny), sl]
        total = total + (e[x + 1, pl.ds(0, ny), sl] + e[x + 1, pl.ds(2, ny), sl])
        h = jnp.stack([edge_at(got, x * ny + y, 1) for y in range(ny)])
        low = roll(jnp.where(lane[None] >= nz - 1, h, c), 1)
        high = roll(jnp.where(lane[None] < 1, h, c), -1)
        return c, total + (low + high)

    def fine_edges(p, sl):
        return join(lambda s: zrecv[p, s, sl], 1)

    def fine_pack(p, sl):
        zsend[p, sl] = pack(lambda x, y: fine[p][x + 1, y + 1, sl], nx, ny, 1)

    def slab(k, i):
        return pl.ds(pl.multiple_of(k * width + i * 8, 8), 8)

    pltpu.make_async_copy(
        fine[ORB].at[pl.ds(1, nx), pl.ds(1, ny)],
        fine[ORB].at[pl.ds(1, nx), pl.ds(1, ny)],
        load_sem.at[0],
    ).wait()
    pl.semaphore_wait(barrier, len(peers) + ycount)

    def start_near(k, carry):
        down, up, *rest = fine_moves(ORB, k)

        @pl.when(gy > 0)
        def _():
            go([down], 0, k)

        @pl.when(gy < ylast)
        def _():
            go([up], 0, k)

        go(rest[:2], 0, k)
        return carry

    def start_far(k, carry):
        down, up, *_ = fine_moves(ORB, k)

        @pl.when(gy == 0)
        def _():
            go([down], 0, k)

        @pl.when(gy == ylast)
        def _():
            go([up], 0, k)

        return carry

    lax.fori_loop(0, early, start_near, 0)
    for end, step, sem in ((0, 1, 0), (ylast, -1, 1)):
        first, stop = end + step, ylast - end

        @pl.when((gy != end) & (gy != first))
        def _():
            pl.semaphore_wait(token.at[sem], 1)

        @pl.when((gy != end) & (gy != stop))
        def _():
            signal(token.at[sem], {"gy": gy + step})

    lax.fori_loop(0, early, start_far, 0)

    def start_all(k, carry):
        start_far(k, carry)
        return start_near(k, carry)

    lax.fori_loop(early, chunks, start_all, 0)

    def start_z(k, carry):
        def inner(i, c):
            fine_pack(ORB, slab(k, i))
            return c

        lax.fori_loop(0, groups, inner, 0)
        go(fine_moves(ORB, k)[4:], 0, k)
        return carry

    lax.fori_loop(0, chunks, start_z, 0)

    for small in smalls:
        small.wait()
    for g in range(bands // 8):
        m = jnp.zeros((8, nz), jnp.float32)
        s = jnp.ones((8, nz), jnp.float32)
        for j in range(8):
            m = jnp.where(sub == j, centre[g * 8 + j], m)
            s = jnp.where(sub == j, half_width[g * 8 + j], s)
        band_a[pl.ds(g * 8, 8)] = 3.0 - m
        band_i[pl.ds(g * 8, 8)] = 1.0 / s
    for x in range(nx):
        for y in range(ny):
            pot_b[x, y] = jnp.broadcast_to(pot[x, pl.ds(y, 1), :], (8, nz))
    for x2 in range(qx):
        for y2 in range(qy):
            quad = jnp.zeros((8, nz), jnp.float32)
            for hx in range(2):
                for hy in range(2):
                    x, y = 2 * x2 + hx, 2 * y2 + hy
                    v = pot_b[2 * x, 2 * y] + pot_b[2 * x + 1, 2 * y]
                    v = v + (pot_b[2 * x, 2 * y + 1] + pot_b[2 * x + 1, 2 * y + 1])
                    one = 0.125 * pair_sum(v, 1)
                    quad = quad + one
                    d1 = 0.75 + one + shift_mass
                    d1_b[x, y] = d1
                    r1_b[x + 1, y + 1] = jacobi_weight / d1
            r2_b[x2 + 1, y2 + 1] = jacobi_weight / (0.1875 + 0.125 * pair_sum(quad, 2) + shift_mass)
    for j, (x, y) in enumerate([(0, None), (mx - 1, None), (None, 0), (None, my - 1)]):
        for i in range(my if y is None else mx):
            cx, cy = (x, i) if y is None else (i, y)
            r_sent[j, pl.ds(i, 1)] = r1_b[cx + 1, cy + 1][0:1]
    for j, (x, y) in enumerate([(0, None), (qx - 1, None), (None, 0), (None, qy - 1)]):
        base = my if y is None else mx
        for i in range(qy if y is None else qx):
            cx, cy = (x, i) if y is None else (i, y)
            r_sent[j, pl.ds(base + i, 1)] = r2_b[cx + 1, cy + 1][0:1]
    r_sent[4, pl.ds(0, 1)] = pack(lambda x, y: r1_b[x + 1, y + 1], mx, my, 4)[0:1]
    r_sent[4, pl.ds(1, 1)] = pack(lambda x, y: r2_b[x + 1, y + 1], qx, qy, 8)[0:1]

    go(r_moves(), 5, at_r)

    def step_first(k, carry):
        arrive(fine_moves(ORB, k), k)

        def inner(i, c):
            sl = slab(k, i)
            got = fine_edges(ORB, sl)
            a, f = band_a[sl], band_i[sl]
            for x in range(nx):
                v, total = around(ORB, sl, got, x)
                fine[FIRST][x + 1, pl.ds(1, ny), sl] = ((pot_b[x] + a) * v - 0.5 * total) * f
            fine_pack(FIRST, sl)
            return c

        lax.fori_loop(0, groups, inner, 0)
        go_faces(fine_moves(FIRST, k), 1, chunks + k)
        return carry

    lax.fori_loop(0, chunks, step_first, 0)

    arrive(r_moves(), at_r)
    for i in range(my):
        for j, x in ((0, 0), (1, mx + 1)):
            r1_b[x, i + 1] = jnp.broadcast_to(r_got[j, pl.ds(i, 1)], (8, nz))
    for i in range(mx):
        for j, y in ((2, 0), (3, my + 1)):
            r1_b[i + 1, y] = jnp.broadcast_to(r_got[j, pl.ds(i, 1)], (8, nz))
    for i in range(qy):
        for j, x in ((0, 0), (1, qx + 1)):
            r2_b[x, i + 1] = jnp.broadcast_to(r_got[j, pl.ds(my + i, 1)], (8, nz))
    for i in range(qx):
        for j, y in ((2, 0), (3, qy + 1)):
            r2_b[i + 1, y] = jnp.broadcast_to(r_got[j, pl.ds(mx + i, 1)], (8, nz))

    def r_edge(row, w):
        return join(lambda s: jnp.broadcast_to(r_got[4 + s, pl.ds(row, 1)], (8, nz)), w)

    def step_second(k, carry):
        arrive(fine_moves(FIRST, k), chunks + k)
        packed = pl.ds(pl.multiple_of(k * 8, 8), 8)

        def inner(i, c):
            sl = slab(k, i)
            mine = (lane & 1) == i
            got = fine_edges(FIRST, sl)
            a, f = band_a[sl], 2.0 * band_i[sl]
            for x2 in range(mx):
                both = None
                for x in (2 * x2, 2 * x2 + 1):
                    v, total = around(FIRST, sl, got, x)
                    v = ((pot_b[x] + a) * v - 0.5 * total) * f - fine[ORB][x + 1, pl.ds(1, ny), sl]
                    second[x, :, sl] = v
                    both = v if both is None else both + v
                for y2 in range(my):
                    s = 0.5 * pair_sum(both[2 * y2] + both[2 * y2 + 1], 1)
                    one_a[x2 + 2, y2 + 2, packed] = jnp.where(
                        mine, r1_b[x2 + 1, y2 + 1] * s, one_a[x2 + 2, y2 + 2, packed]
                    )
            return c

        lax.fori_loop(0, groups, inner, 0)
        one_edge[packed] = pack(lambda x, y: one_a[x + 2, y + 2, packed], mx, my, 4)
        go_deep(one_moves(k), 2, at_one + k)
        return carry

    lax.fori_loop(0, chunks, step_second, 0)

    def step_residue(k, carry):
        arrive(one_moves(k), at_one + k)
        packed = pl.ds(pl.multiple_of(k * 8, 8), 8)
        rows = pl.ds(pl.multiple_of(lax.div(k, 2) * 8, 8), 8)
        mine = ((lane >> 1) & 1) == lax.rem(k, 2)
        ends = [join(lambda s, j=j: one_got[s, j, packed], 4) for j in range(5)]
        halo = sweep_edges(one_edge[packed], ends, r_edge(0, 4), mx, my, 4, 0.125)
        one_halo[packed] = halo
        sweep_wide(
            one_a, one_b, ends, lambda x, y: r1_b[x + 1, y + 1], packed, mx, my, 4, 0.125
        )
        for x2 in range(qx):
            for y2 in range(qy):
                acc = None
                for x in (2 * x2, 2 * x2 + 1):
                    for y in (2 * y2, 2 * y2 + 1):
                        h = edge_at(halo, x * my + y, 4)
                        c, total = total_of(one_b, x, y, packed, h, 2)
                        d = d1_b[x, y]
                        source = one_a[x + 2, y + 2, packed] * (d * (1.0 / jacobi_weight))
                        v = source - d * c + 0.125 * total
                        acc = v if acc is None else acc + v
                s = 0.5 * pair_sum(acc, 2)
                two_a[x2 + 2, y2 + 2, rows] = jnp.where(
                    mine, r2_b[x2 + 1, y2 + 1] * s, two_a[x2 + 2, y2 + 2, rows]
                )
        return carry

    def pair_residue(k, carry):
        lax.fori_loop(2 * k, 2 * k + 2, step_residue, 0)
        rows = pl.ds(pl.multiple_of(k * 8, 8), 8)
        two_edge[rows] = pack(lambda x, y: two_a[x + 2, y + 2, rows], qx, qy, 8)
        go_deep(two_moves(k), 3, at_two + k)
        return carry

    lax.fori_loop(0, pairs, pair_residue, 0)

    def step_two(k, carry):
        arrive(two_moves(k), at_two + k)
        rows = pl.ds(pl.multiple_of(k * 8, 8), 8)
        ends = [join(lambda s, j=j: two_got[s, j, rows], 8) for j in range(5)]
        halo = sweep_edges(two_edge[rows], ends, r_edge(1, 8), qx, qy, 8, 0.03125)
        sweep_wide(
            two_a, two_b, ends, lambda x, y: r2_b[x + 1, y + 1], rows, qx, qy, 8, 0.03125
        )
        for x in range(qx):
            for y in range(qy):
                c, total = total_of(two_b, x, y, rows, edge_at(halo, x * qy + y, 8), 4)
                two_c[x + 1, y + 1, rows] = (
                    (1.0 - jacobi_weight) * c
                    + two_a[x + 2, y + 2, rows]
                    + 0.03125 * r2_b[x + 1, y + 1] * total
                )
        last_edge[rows] = pack(lambda x, y: two_c[x + 1, y + 1, rows], qx, qy, 4)
        go_faces(last_moves(k), 4, at_last + k)
        return carry

    lax.fori_loop(0, pairs, step_two, 0)

    def step_last(k, half):
        rows = pl.ds(pl.multiple_of(k * 8, 8), 8)
        packed = pl.ds(pl.multiple_of(k * 16 + half * 8, 8), 8)
        left = (lane & 2) == 0

        def spread(v):
            return jnp.where(left, v, roll(v, 2)) if half == 0 else jnp.where(left, roll(v, -2), v)

        coarse = {}
        for x in range(-1, qx + 1):
            for y in range(-1, qy + 1):
                if 0 <= x < qx or 0 <= y < qy:
                    coarse[x, y] = spread(two_c[x + 1, y + 1, rows])
        got = join(lambda s: last_got[s, rows], 4)
        ends = {
            (x, y): spread(edge_at(got, x * qy + y, 4)) for x in range(qx) for y in range(qy)
        }
        halo = one_halo[packed]

        def at(x, y):
            return one_b[x + 1, y + 1, packed] + coarse[(x + 2) // 2 - 1, (y + 2) // 2 - 1]

        for x in range(mx):
            for y in range(my):
                c = at(x, y)
                total = (at(x - 1, y) + at(x + 1, y)) + (at(x, y - 1) + at(x, y + 1))
                h = edge_at(halo, x * my + y, 4) + ends[x // 2, y // 2]
                total = total + along_z(c, h, 2)
                v = (1.0 - jacobi_weight) * c + one_a[x + 2, y + 2, packed]
                v = v + 0.125 * r1_b[x + 1, y + 1] * total
                odd = (lane & 1) == 1
                for i, w in enumerate((jnp.where(odd, roll(v, 1), v), jnp.where(odd, v, roll(v, -1)))):
                    sl = slab(2 * k + half, i)
                    for hx in range(2):
                        for hy in range(2):
                            fx, fy = 2 * x + hx, 2 * y + hy
                            second[fx, fy, sl] = second[fx, fy, sl] + w

    def finish(k, carry):
        arrive(last_moves(k), at_last + k)
        for half in range(2):
            step_last(k, half)
        return carry

    lax.fori_loop(0, pairs, finish, 0)

    leave(fine_moves(ORB, 0), chunks, 0)
    leave(fine_moves(FIRST, 0), chunks, 1)
    leave(one_moves(0), chunks, 2)
    leave(two_moves(0), pairs, 3)
    leave(last_moves(0), pairs, 4)
    leave(r_moves(), 1, 5)


def store(filtered, out, sem):
    nx, ny = filtered.shape[:2]

    def line(x, c):
        for y in range(ny):
            pltpu.make_async_copy(filtered.at[x, y], out.at[:, x, y], sem).start()
        return c

    lax.fori_loop(0, nx, line, 0)
    pltpu.make_async_copy(filtered, filtered, sem).wait()


def local(sizes, chunks, orbitals, potential, centre, half_width):
    bands, nx, ny, nz = orbitals.shape
    sides = 2 if sizes["gz"] > 2 else 1
    pairs = chunks // 2

    def f32(*shape):
        return pltpu.VMEM(shape, jnp.float32)

    def padded(cut, halo):
        return f32(nx // cut + 2 * halo, ny // cut + 2 * halo, bands if cut == 1 else bands // cut, nz)

    dma = pltpu.SemaphoreType.DMA
    scratch = [padded(1, 1)] * 2 + [padded(2, 2), padded(2, 1), padded(4, 2), padded(4, 1), padded(4, 1)]
    scratch += [
        f32(2, bands, nz),
        f32(2, sides, bands, nz),
        f32(bands // 2, nz),
        f32(sides, 5, bands // 2, nz),
        f32(bands // 2, nz),
        f32(bands // 4, nz),
        f32(sides, 5, bands // 4, nz),
        f32(bands // 4, nz),
        f32(sides, bands // 4, nz),
        f32(bands, nz),
        f32(bands, nz),
        f32(nx, ny, 8, nz),
        f32(nx // 2, ny // 2, 8, nz),
        f32(nx // 2 + 2, ny // 2 + 2, 8, nz),
        f32(nx // 4 + 2, ny // 4 + 2, 8, nz),
        f32(5, 8, nz),
        f32(4 + sides, 8, nz),
        dma((1,)),
        dma((6,)),
        dma((3 * chunks + 2 * pairs + 1,)),
        f32((2 * (nx + ny) + sides) * bands // 8, 8, nz),
        pltpu.SMEM((bands,), jnp.float32),
        pltpu.SMEM((bands,), jnp.float32),
        f32(nx, ny, nz),
        dma((3,)),
        pltpu.SemaphoreType.REGULAR((2,)),
    ]
    filtered = pl.pallas_call(
        functools.partial(kernel, sizes, chunks),
        out_shape=pltpu.VMEM((nx, ny, bands, nz), jnp.float32),
        in_specs=[pl.BlockSpec(memory_space=pltpu.HBM)] * 4,
        out_specs=pl.BlockSpec(memory_space=pltpu.VMEM),
        scratch_shapes=scratch,
        compiler_params=pltpu.CompilerParams(
            collective_id=0, has_side_effects=True, vmem_limit_bytes=48 * 1024 * 1024
        ),
    )(*(pltpu.with_memory_space_constraint(v, pltpu.HBM) for v in (centre, half_width, potential, orbitals)))
    return pl.pallas_call(
        store,
        out_shape=jax.ShapeDtypeStruct(orbitals.shape, jnp.float32),
        in_specs=[pl.BlockSpec(memory_space=pltpu.VMEM)],
        out_specs=pl.BlockSpec(memory_space=pltpu.HBM),
        scratch_shapes=[dma(())],
    )(pltpu.with_memory_space_constraint(filtered, pltpu.VMEM))


def solution(mesh):
    in_specs = (P(None, "gx", "gy", "gz"), P("gx", "gy", "gz"), P(), P())
    out_specs = P(None, "gx", "gy", "gz")
    body = functools.partial(local, dict(mesh.shape), 4)
    return jax.shard_map(body, mesh=mesh, in_specs=in_specs, out_specs=out_specs, check_vma=False)
```

```python
import functools
import math

import jax
import jax.numpy as jnp
from jax import lax
from jax.experimental import pallas as pl
from jax.experimental.pallas import tpu as pltpu
from jax.sharding import PartitionSpec as P

shift_mass = 0.05
jacobi_weight = 2.0 / 3.0
MESH = pl.DeviceIdType.MESH
ORB, FIRST = range(2)


def kernel(sizes, chunks, centre_in, half_width_in, pot_in, orbitals, second, *scratch):
    fine = scratch[0:2]
    one_a, one_b, two_a, two_b, two_c = scratch[2:7]
    zsend, zrecv = scratch[7:9]
    one_edge, one_got, one_halo, two_edge, two_got, last_edge, last_got = scratch[9:16]
    band_a, band_i, pot_b, d1_b, r1_b, r2_b, r_sent, r_got = scratch[16:24]
    load_sem, send_sem, recv_sem, tally = scratch[24:28]
    centre, half_width, pot, small_sem, token, relay_edge = scratch[28:34]
    bands, nx, ny, nz = second.shape[2], second.shape[0], second.shape[1], second.shape[3]
    width = bands // chunks
    groups = width // 8
    pairs = chunks // 2
    early = chunks // 2
    relayed = 2 * (pairs - 1)
    mx, my, qx, qy = nx // 2, ny // 2, nx // 4, ny // 4
    sides = 2 if sizes["gz"] > 2 else 1
    at_one, at_two = 2 * chunks, 3 * chunks
    at_last, at_r = at_two + pairs, at_two + 2 * pairs
    at_relay = at_r + 1
    lane = lax.broadcasted_iota(jnp.int32, (8, nz), 1)
    sub = lax.broadcasted_iota(jnp.int32, (8, nz), 0)

    near = {}
    for axis in ("gx", "gy", "gz"):
        me, n = lax.axis_index(axis), sizes[axis]
        near[axis] = (lax.rem(me + n - 1, n), lax.rem(me + 1, n))
    zpeers = [near["gz"][1], near["gz"][0]][:sides]
    gy, ylast = lax.axis_index("gy"), sizes["gy"] - 1
    peers = [{"gx": v} for v in near["gx"]] + [{"gz": v} for v in zpeers]

    def signal(sem, to):
        pl.semaphore_signal(sem, inc=1, device_id=to, device_id_type=MESH)

    barrier = pltpu.get_barrier_semaphore()
    for peer in peers:
        signal(barrier, peer)

    @pl.when(gy > 0)
    def _():
        signal(barrier, {"gy": gy - 1})

    @pl.when(gy < ylast)
    def _():
        signal(barrier, {"gy": gy + 1})

    ycount = lax.div(gy + ylast, ylast + 1) + lax.div(2 * ylast - gy, ylast + 1)

    smalls = [
        pltpu.make_async_copy(src, dst, small_sem.at[j])
        for j, (src, dst) in enumerate(
            [(centre_in, centre), (half_width_in, half_width), (pot_in, pot)]
        )
    ]
    for small in smalls:
        small.start()

    def load(x, c):
        for y in range(ny):
            pltpu.make_async_copy(
                orbitals.at[:, x, y], fine[ORB].at[x + 1, y + 1], load_sem.at[0]
            ).start()
        return c

    lax.fori_loop(0, nx, load, 0)

    def tiles(moves):
        return sum(math.prod(src.shape) for src, _, _ in moves) // (8 * nz)

    def take(n, sem):
        whole = tally.at[pl.ds(0, n)]
        pltpu.make_async_copy(whole, whole, sem).wait()

    def go(moves, sent, got):
        for src, dst, to in moves:
            pltpu.make_async_remote_copy(
                src_ref=src,
                dst_ref=dst,
                send_sem=send_sem.at[sent],
                recv_sem=recv_sem.at[got],
                device_id=to,
                device_id_type=MESH,
            ).start()

    def go_split(downs, ups, rest, sent, got):
        @pl.when(gy == ylast)
        def _():
            go(ups + downs, sent, got)

        @pl.when(gy != ylast)
        def _():
            go(downs + ups, sent, got)

        go(rest, sent, got)

    def go_faces(moves, sent, got):
        go_split(moves[:1], moves[1:2], moves[2:], sent, got)

    def go_deep(moves, sent, got):
        downs, ups = [moves[0], *moves[4:6]], [moves[1], *moves[6:8]]
        rest = moves[2:4]
        for s in range(sides):
            ends = moves[8 + 5 * s : 13 + 5 * s]
            rest, ups, downs = rest + ends[:3], ups + ends[3:4], downs + ends[4:]
        go_split(downs, ups, rest, sent, got)

    def arrive(moves, got):
        take(tiles(moves), recv_sem.at[got])

    def leave(moves, times, sent):
        take(times * tiles(moves), send_sem.at[sent])

    def fine_moves(p, k):
        e = fine[p]
        rows = pl.ds(pl.multiple_of(k * width, 8), width)
        ys, xs = pl.ds(1, ny), pl.ds(1, nx)
        moves = [
            (e.at[xs, 1, rows], e.at[xs, ny + 1, rows], {"gy": near["gy"][0]}),
            (e.at[xs, ny, rows], e.at[xs, 0, rows], {"gy": near["gy"][1]}),
            (e.at[1, ys, rows], e.at[nx + 1, ys, rows], {"gx": near["gx"][0]}),
            (e.at[nx, ys, rows], e.at[0, ys, rows], {"gx": near["gx"][1]}),
        ]
        for s, to in enumerate(zpeers):
            moves.append((zsend.at[p, rows], zrecv.at[p, s, rows], {"gz": to}))
        return moves

    def deep_moves(e, edge, got, k):
        ax, ay = e.shape[0] - 4, e.shape[1] - 4
        rows = pl.ds(pl.multiple_of(k * 8, 8), 8)
        ys, xs = pl.ds(2, ay), pl.ds(2, ax)
        lo, hix, hiy, topx, topy = pl.ds(0, 2), pl.ds(ax, 2), pl.ds(ay, 2), pl.ds(ax + 2, 2), pl.ds(ay + 2, 2)
        two = pl.ds(2, 2)
        (xm, xp), (ym, yp) = near["gx"], near["gy"]
        moves = [
            (e.at[xs, two, rows], e.at[xs, topy, rows], {"gy": ym}),
            (e.at[xs, hiy, rows], e.at[xs, lo, rows], {"gy": yp}),
            (e.at[two, ys, rows], e.at[topx, ys, rows], {"gx": xm}),
            (e.at[hix, ys, rows], e.at[lo, ys, rows], {"gx": xp}),
            (e.at[2, 2, rows], e.at[ax + 2, ay + 2, rows], {"gx": xm, "gy": ym}),
            (e.at[ax + 1, 2, rows], e.at[1, ay + 2, rows], {"gx": xp, "gy": ym}),
            (e.at[2, ay + 1, rows], e.at[ax + 2, 1, rows], {"gx": xm, "gy": yp}),
            (e.at[ax + 1, ay + 1, rows], e.at[1, 1, rows], {"gx": xp, "gy": yp}),
        ]
        for s, z in enumerate(zpeers):
            for j, to in enumerate([{}, {"gx": xp}, {"gx": xm}, {"gy": yp}, {"gy": ym}]):
                moves.append((edge.at[rows], got.at[s, j, rows], {"gz": z, **to}))
        return moves

    def early_moves(k):
        moves = one_moves(k)
        keep = moves[:4]
        for s in range(sides):
            keep += moves[8 + 5 * s : 11 + 5 * s]
        return keep

    def relay_moves(k):
        e = one_a
        rows = pl.ds(pl.multiple_of(k * 8, 8), 8)
        xm, xp = near["gx"]
        moves = []
        for y in (1, my + 2):
            moves.append((e.at[2, y, rows], e.at[mx + 2, y, rows], {"gx": xm}))
            moves.append((e.at[mx + 1, y, rows], e.at[1, y, rows], {"gx": xp}))
        for s, z in enumerate(zpeers):
            for j in (3, 4):
                moves.append((relay_edge.at[rows], one_got.at[s, j, rows], {"gz": z}))
        return moves

    def last_moves(k):
        e = two_c
        rows = pl.ds(pl.multiple_of(k * 8, 8), 8)
        ys, xs = pl.ds(1, qy), pl.ds(1, qx)
        moves = [
            (e.at[xs, 1, rows], e.at[xs, qy + 1, rows], {"gy": near["gy"][0]}),
            (e.at[xs, qy, rows], e.at[xs, 0, rows], {"gy": near["gy"][1]}),
            (e.at[1, ys, rows], e.at[qx + 1, ys, rows], {"gx": near["gx"][0]}),
            (e.at[qx, ys, rows], e.at[0, ys, rows], {"gx": near["gx"][1]}),
        ]
        for s, to in enumerate(zpeers):
            moves.append((last_edge.at[rows], last_got.at[s, rows], {"gz": to}))
        return moves

    def r_moves():
        moves = [
            (r_sent.at[0], r_got.at[1], {"gx": near["gx"][0]}),
            (r_sent.at[1], r_got.at[0], {"gx": near["gx"][1]}),
            (r_sent.at[2], r_got.at[3], {"gy": near["gy"][0]}),
            (r_sent.at[3], r_got.at[2], {"gy": near["gy"][1]}),
        ]
        for s, to in enumerate(zpeers):
            moves.append((r_sent.at[4], r_got.at[4 + s], {"gz": to}))
        return moves

    def one_moves(k):
        return deep_moves(one_a, one_edge, one_got, k)

    def two_moves(k):
        return deep_moves(two_a, two_edge, two_got, k)

    def roll(v, shift):
        return pltpu.roll(v, shift % nz, v.ndim - 1)

    def pack(get, ax, ay, w):
        acc = jnp.zeros((8, nz), jnp.float32)
        for x in range(ax):
            for y in range(ay):
                at = 2 * w * (x * ay + y)
                here = (lane >= at) & (lane < at + 2 * w)
                acc = jnp.where(here, roll(get(x, y), at + w), acc)
        return acc

    def edge_at(got, spot, w):
        return roll(got, -(2 * w * spot) - w)

    def join(got, w):
        if sides == 1:
            return got(0)
        return jnp.where((lane & (2 * w - 1)) < w, got(0), got(1))

    def along_z(v, h, w):
        low = roll(jnp.where(lane >= nz - w, h, v), w)
        high = roll(jnp.where(lane < w, h, v), -w)
        return low + high

    def pair_sum(v, w):
        even = (lane & (2 * w - 1)) < w
        return v + jnp.where(even, roll(v, -w), roll(v, w))

    def sweep_edges(own, ends, r, ax, ay, w, coupling):
        cell = w // 2
        mid, xm, xp, ym, yp = ends
        sy, sx = 2 * w, 2 * w * ay
        spot = lane // sy
        yi, xi = spot % ay, spot // ay
        z = jnp.where(
            (lane & (2 * w - 1)) >= w,
            roll(mid, -cell) + roll(own, cell),
            roll(mid, cell) + roll(own, -cell),
        )
        total = z + jnp.where(yi == ay - 1, roll(yp, sy * (ay - 1)), roll(mid, -sy))
        total = total + jnp.where(yi == 0, roll(ym, -sy * (ay - 1)), roll(mid, sy))
        total = total + jnp.where(xi == ax - 1, roll(xp, sx * (ax - 1)), roll(mid, -sx))
        total = total + jnp.where(xi == 0, roll(xm, -sx * (ax - 1)), roll(mid, sx))
        return (2.0 - jacobi_weight) * mid + coupling * r * total

    def sweep_wide(src, dst, ends, r_at, rows, ax, ay, w, coupling):
        mid, xm, xp, ym, yp = ends
        cells = [(x, y, mid, x * ay + y) for x in range(ax) for y in range(ay)]
        cells += [(-1, y, xm, (ax - 1) * ay + y) for y in range(ay)]
        cells += [(ax, y, xp, y) for y in range(ay)]
        cells += [(x, -1, ym, x * ay + ay - 1) for x in range(ax)]
        cells += [(x, ay, yp, x * ay) for x in range(ax)]
        for x, y, got, spot in cells:
            c = src[x + 2, y + 2, rows]
            total = (src[x + 1, y + 2, rows] + src[x + 3, y + 2, rows]) + (
                src[x + 2, y + 1, rows] + src[x + 2, y + 3, rows]
            )
            total = total + along_z(c, edge_at(got, spot, w), w // 2)
            dst[x + 1, y + 1, rows] = (2.0 - jacobi_weight) * c + coupling * r_at(x, y) * total

    def total_of(e, x, y, rows, h, w):
        c = e[x + 1, y + 1, rows]
        total = (e[x, y + 1, rows] + e[x + 2, y + 1, rows]) + (
            e[x + 1, y, rows] + e[x + 1, y + 2, rows]
        )
        return c, total + along_z(c, h, w)

    def around(p, sl, got, x):
        e = fine[p]
        c = e[x + 1, pl.ds(1, ny), sl]
        total = e[x, pl.ds(1, ny), sl] + e[x + 2, pl.ds(1, ny), sl]
        total = total + (e[x + 1, pl.ds(0, ny), sl] + e[x + 1, pl.ds(2, ny), sl])
        h = jnp.stack([edge_at(got, x * ny + y, 1) for y in range(ny)])
        low = roll(jnp.where(lane[None] >= nz - 1, h, c), 1)
        high = roll(jnp.where(lane[None] < 1, h, c), -1)
        return c, total + (low + high)

    def fine_edges(p, sl):
        return join(lambda s: zrecv[p, s, sl], 1)

    def fine_pack(p, sl):
        zsend[p, sl] = pack(lambda x, y: fine[p][x + 1, y + 1, sl], nx, ny, 1)

    def slab(k, i):
        return pl.ds(pl.multiple_of(k * width + i * 8, 8), 8)

    pltpu.make_async_copy(
        fine[ORB].at[pl.ds(1, nx), pl.ds(1, ny)],
        fine[ORB].at[pl.ds(1, nx), pl.ds(1, ny)],
        load_sem.at[0],
    ).wait()
    pl.semaphore_wait(barrier, len(peers) + ycount)

    def start_near(k, carry):
        down, up, *rest = fine_moves(ORB, k)

        @pl.when(gy > 0)
        def _():
            go([down], 0, k)

        @pl.when(gy < ylast)
        def _():
            go([up], 0, k)

        go(rest[:2], 0, k)
        return carry

    def start_far(k, carry):
        down, up, *_ = fine_moves(ORB, k)

        @pl.when(gy == 0)
        def _():
            go([down], 0, k)

        @pl.when(gy == ylast)
        def _():
            go([up], 0, k)

        return carry

    lax.fori_loop(0, early, start_near, 0)
    for end, step, sem in ((0, 1, 0), (ylast, -1, 1)):
        first, stop = end + step, ylast - end

        @pl.when((gy != end) & (gy != first))
        def _():
            pl.semaphore_wait(token.at[sem], 1)

        @pl.when((gy != end) & (gy != stop))
        def _():
            signal(token.at[sem], {"gy": gy + step})

    lax.fori_loop(0, early, start_far, 0)

    def start_all(k, carry):
        start_far(k, carry)
        return start_near(k, carry)

    lax.fori_loop(early, chunks, start_all, 0)

    def start_z(k, carry):
        def inner(i, c):
            fine_pack(ORB, slab(k, i))
            return c

        lax.fori_loop(0, groups, inner, 0)
        go(fine_moves(ORB, k)[4:], 0, k)
        return carry

    lax.fori_loop(0, chunks, start_z, 0)

    for small in smalls:
        small.wait()
    for g in range(bands // 8):
        m = jnp.zeros((8, nz), jnp.float32)
        s = jnp.ones((8, nz), jnp.float32)
        for j in range(8):
            m = jnp.where(sub == j, centre[g * 8 + j], m)
            s = jnp.where(sub == j, half_width[g * 8 + j], s)
        band_a[pl.ds(g * 8, 8)] = 3.0 - m
        band_i[pl.ds(g * 8, 8)] = 1.0 / s
    for x in range(nx):
        for y in range(ny):
            pot_b[x, y] = jnp.broadcast_to(pot[x, pl.ds(y, 1), :], (8, nz))
    for x2 in range(qx):
        for y2 in range(qy):
            quad = jnp.zeros((8, nz), jnp.float32)
            for hx in range(2):
                for hy in range(2):
                    x, y = 2 * x2 + hx, 2 * y2 + hy
                    v = pot_b[2 * x, 2 * y] + pot_b[2 * x + 1, 2 * y]
                    v = v + (pot_b[2 * x, 2 * y + 1] + pot_b[2 * x + 1, 2 * y + 1])
                    one = 0.125 * pair_sum(v, 1)
                    quad = quad + one
                    d1 = 0.75 + one + shift_mass
                    d1_b[x, y] = d1
                    r1_b[x + 1, y + 1] = jacobi_weight / d1
            r2_b[x2 + 1, y2 + 1] = jacobi_weight / (0.1875 + 0.125 * pair_sum(quad, 2) + shift_mass)
    for j, (x, y) in enumerate([(0, None), (mx - 1, None), (None, 0), (None, my - 1)]):
        for i in range(my if y is None else mx):
            cx, cy = (x, i) if y is None else (i, y)
            r_sent[j, pl.ds(i, 1)] = r1_b[cx + 1, cy + 1][0:1]
    for j, (x, y) in enumerate([(0, None), (qx - 1, None), (None, 0), (None, qy - 1)]):
        base = my if y is None else mx
        for i in range(qy if y is None else qx):
            cx, cy = (x, i) if y is None else (i, y)
            r_sent[j, pl.ds(base + i, 1)] = r2_b[cx + 1, cy + 1][0:1]
    r_sent[4, pl.ds(0, 1)] = pack(lambda x, y: r1_b[x + 1, y + 1], mx, my, 4)[0:1]
    r_sent[4, pl.ds(1, 1)] = pack(lambda x, y: r2_b[x + 1, y + 1], qx, qy, 8)[0:1]

    go(r_moves(), 7, at_r)

    def step_first(k, carry):
        arrive(fine_moves(ORB, k), k)

        def inner(i, c):
            sl = slab(k, i)
            got = fine_edges(ORB, sl)
            a, f = band_a[sl], band_i[sl]
            for x in range(nx):
                v, total = around(ORB, sl, got, x)
                fine[FIRST][x + 1, pl.ds(1, ny), sl] = ((pot_b[x] + a) * v - 0.5 * total) * f
            fine_pack(FIRST, sl)
            return c

        lax.fori_loop(0, groups, inner, 0)
        go_faces(fine_moves(FIRST, k), 1, chunks + k)
        return carry

    lax.fori_loop(0, chunks, step_first, 0)

    arrive(r_moves(), at_r)
    for i in range(my):
        for j, x in ((0, 0), (1, mx + 1)):
            r1_b[x, i + 1] = jnp.broadcast_to(r_got[j, pl.ds(i, 1)], (8, nz))
    for i in range(mx):
        for j, y in ((2, 0), (3, my + 1)):
            r1_b[i + 1, y] = jnp.broadcast_to(r_got[j, pl.ds(i, 1)], (8, nz))
    for i in range(qy):
        for j, x in ((0, 0), (1, qx + 1)):
            r2_b[x, i + 1] = jnp.broadcast_to(r_got[j, pl.ds(my + i, 1)], (8, nz))
    for i in range(qx):
        for j, y in ((2, 0), (3, qy + 1)):
            r2_b[i + 1, y] = jnp.broadcast_to(r_got[j, pl.ds(mx + i, 1)], (8, nz))

    def r_edge(row, w):
        return join(lambda s: jnp.broadcast_to(r_got[4 + s, pl.ds(row, 1)], (8, nz)), w)

    def step_second(k, carry):
        arrive(fine_moves(FIRST, k), chunks + k)
        packed = pl.ds(pl.multiple_of(k * 8, 8), 8)

        def inner(i, c):
            sl = slab(k, i)
            mine = (lane & 1) == i
            got = fine_edges(FIRST, sl)
            a, f = band_a[sl], 2.0 * band_i[sl]
            for x2 in range(mx):
                both = None
                for x in (2 * x2, 2 * x2 + 1):
                    v, total = around(FIRST, sl, got, x)
                    v = ((pot_b[x] + a) * v - 0.5 * total) * f - fine[ORB][x + 1, pl.ds(1, ny), sl]
                    second[x, :, sl] = v
                    both = v if both is None else both + v
                for y2 in range(my):
                    s = 0.5 * pair_sum(both[2 * y2] + both[2 * y2 + 1], 1)
                    one_a[x2 + 2, y2 + 2, packed] = jnp.where(
                        mine, r1_b[x2 + 1, y2 + 1] * s, one_a[x2 + 2, y2 + 2, packed]
                    )
            return c

        lax.fori_loop(0, groups, inner, 0)
        one_edge[packed] = pack(lambda x, y: one_a[x + 2, y + 2, packed], mx, my, 4)
        return carry

    def second_early(k, carry):
        step_second(k, carry)
        go_faces(early_moves(k), 2, at_one + k)
        return carry

    lax.fori_loop(0, relayed, second_early, 0)

    def second_late(k, carry):
        step_second(k, carry)
        go_deep(one_moves(k), 3, at_one + k)
        return carry

    lax.fori_loop(relayed, chunks, second_late, 0)

    def relay(k, carry):
        arrive(early_moves(k), at_one + k)
        rows = pl.ds(pl.multiple_of(k * 8, 8), 8)
        spots = [(x, y) for x in range(mx) for y in (0, my - 1)]
        acc = jnp.zeros((8, nz), jnp.float32)
        for x, y in spots:
            at = 8 * (x * my + y)
            here = (lane >= at) & (lane < at + 8)
            acc = jnp.where(here, roll(one_a[x + 2, my + 2 if y == 0 else 1, rows], at + 4), acc)
        relay_edge[rows] = acc
        go(relay_moves(k), 4, at_relay + k)
        return carry

    lax.fori_loop(0, relayed, relay, 0)

    def step_residue(k, carry):
        packed = pl.ds(pl.multiple_of(k * 8, 8), 8)
        rows = pl.ds(pl.multiple_of(lax.div(k, 2) * 8, 8), 8)
        mine = ((lane >> 1) & 1) == lax.rem(k, 2)
        ends = [join(lambda s, j=j: one_got[s, j, packed], 4) for j in range(5)]
        halo = sweep_edges(one_edge[packed], ends, r_edge(0, 4), mx, my, 4, 0.125)
        one_halo[packed] = halo
        sweep_wide(
            one_a, one_b, ends, lambda x, y: r1_b[x + 1, y + 1], packed, mx, my, 4, 0.125
        )
        for x2 in range(qx):
            for y2 in range(qy):
                acc = None
                for x in (2 * x2, 2 * x2 + 1):
                    for y in (2 * y2, 2 * y2 + 1):
                        h = edge_at(halo, x * my + y, 4)
                        c, total = total_of(one_b, x, y, packed, h, 2)
                        d = d1_b[x, y]
                        source = one_a[x + 2, y + 2, packed] * (d * (1.0 / jacobi_weight))
                        v = source - d * c + 0.125 * total
                        acc = v if acc is None else acc + v
                s = 0.5 * pair_sum(acc, 2)
                two_a[x2 + 2, y2 + 2, rows] = jnp.where(
                    mine, r2_b[x2 + 1, y2 + 1] * s, two_a[x2 + 2, y2 + 2, rows]
                )
        return carry

    def residue_early(k, carry):
        arrive(relay_moves(k), at_relay + k)
        return step_residue(k, carry)

    def send_two(k, carry):
        rows = pl.ds(pl.multiple_of(k * 8, 8), 8)
        two_edge[rows] = pack(lambda x, y: two_a[x + 2, y + 2, rows], qx, qy, 8)
        go_deep(two_moves(k), 5, at_two + k)
        return carry

    def pair_residue(k, carry):
        lax.fori_loop(2 * k, 2 * k + 2, residue_early, 0)
        return send_two(k, carry)

    lax.fori_loop(0, relayed // 2, pair_residue, 0)

    def residue_late(k, carry):
        arrive(one_moves(k), at_one + k)
        return step_residue(k, carry)

    def pair_late(k, carry):
        lax.fori_loop(2 * k, 2 * k + 2, residue_late, 0)
        return send_two(k, carry)

    lax.fori_loop(relayed // 2, pairs, pair_late, 0)

    def step_two(k, carry):
        arrive(two_moves(k), at_two + k)
        rows = pl.ds(pl.multiple_of(k * 8, 8), 8)
        ends = [join(lambda s, j=j: two_got[s, j, rows], 8) for j in range(5)]
        halo = sweep_edges(two_edge[rows], ends, r_edge(1, 8), qx, qy, 8, 0.03125)
        sweep_wide(
            two_a, two_b, ends, lambda x, y: r2_b[x + 1, y + 1], rows, qx, qy, 8, 0.03125
        )
        for x in range(qx):
            for y in range(qy):
                c, total = total_of(two_b, x, y, rows, edge_at(halo, x * qy + y, 8), 4)
                two_c[x + 1, y + 1, rows] = (
                    (1.0 - jacobi_weight) * c
                    + two_a[x + 2, y + 2, rows]
                    + 0.03125 * r2_b[x + 1, y + 1] * total
                )
        last_edge[rows] = pack(lambda x, y: two_c[x + 1, y + 1, rows], qx, qy, 4)
        go_faces(last_moves(k), 6, at_last + k)
        return carry

    lax.fori_loop(0, pairs, step_two, 0)

    def step_last(k, half):
        rows = pl.ds(pl.multiple_of(k * 8, 8), 8)
        packed = pl.ds(pl.multiple_of(k * 16 + half * 8, 8), 8)
        left = (lane & 2) == 0

        def spread(v):
            return jnp.where(left, v, roll(v, 2)) if half == 0 else jnp.where(left, roll(v, -2), v)

        coarse = {}
        for x in range(-1, qx + 1):
            for y in range(-1, qy + 1):
                if 0 <= x < qx or 0 <= y < qy:
                    coarse[x, y] = spread(two_c[x + 1, y + 1, rows])
        got = join(lambda s: last_got[s, rows], 4)
        ends = {
            (x, y): spread(edge_at(got, x * qy + y, 4)) for x in range(qx) for y in range(qy)
        }
        halo = one_halo[packed]

        def at(x, y):
            return one_b[x + 1, y + 1, packed] + coarse[(x + 2) // 2 - 1, (y + 2) // 2 - 1]

        for x in range(mx):
            for y in range(my):
                c = at(x, y)
                total = (at(x - 1, y) + at(x + 1, y)) + (at(x, y - 1) + at(x, y + 1))
                h = edge_at(halo, x * my + y, 4) + ends[x // 2, y // 2]
                total = total + along_z(c, h, 2)
                v = (1.0 - jacobi_weight) * c + one_a[x + 2, y + 2, packed]
                v = v + 0.125 * r1_b[x + 1, y + 1] * total
                odd = (lane & 1) == 1
                for i, w in enumerate((jnp.where(odd, roll(v, 1), v), jnp.where(odd, v, roll(v, -1)))):
                    sl = slab(2 * k + half, i)
                    for hx in range(2):
                        for hy in range(2):
                            fx, fy = 2 * x + hx, 2 * y + hy
                            second[fx, fy, sl] = second[fx, fy, sl] + w

    def finish(k, carry):
        arrive(last_moves(k), at_last + k)
        for half in range(2):
            step_last(k, half)
        return carry

    lax.fori_loop(0, pairs, finish, 0)

    leave(fine_moves(ORB, 0), chunks, 0)
    leave(fine_moves(FIRST, 0), chunks, 1)
    leave(early_moves(0), relayed, 2)
    leave(one_moves(0), chunks - relayed, 3)
    leave(relay_moves(0), relayed, 4)
    leave(two_moves(0), pairs, 5)
    leave(last_moves(0), pairs, 6)
    leave(r_moves(), 1, 7)


def store(filtered, out, sem):
    nx, ny = filtered.shape[:2]

    def line(x, c):
        for y in range(ny):
            pltpu.make_async_copy(filtered.at[x, y], out.at[:, x, y], sem).start()
        return c

    lax.fori_loop(0, nx, line, 0)
    pltpu.make_async_copy(filtered, filtered, sem).wait()


def local(sizes, chunks, orbitals, potential, centre, half_width):
    bands, nx, ny, nz = orbitals.shape
    sides = 2 if sizes["gz"] > 2 else 1
    pairs = chunks // 2

    def f32(*shape):
        return pltpu.VMEM(shape, jnp.float32)

    def padded(cut, halo):
        return f32(nx // cut + 2 * halo, ny // cut + 2 * halo, bands if cut == 1 else bands // cut, nz)

    dma = pltpu.SemaphoreType.DMA
    scratch = [padded(1, 1)] * 2 + [padded(2, 2), padded(2, 1), padded(4, 2), padded(4, 1), padded(4, 1)]
    scratch += [
        f32(2, bands, nz),
        f32(2, sides, bands, nz),
        f32(bands // 2, nz),
        f32(sides, 5, bands // 2, nz),
        f32(bands // 2, nz),
        f32(bands // 4, nz),
        f32(sides, 5, bands // 4, nz),
        f32(bands // 4, nz),
        f32(sides, bands // 4, nz),
        f32(bands, nz),
        f32(bands, nz),
        f32(nx, ny, 8, nz),
        f32(nx // 2, ny // 2, 8, nz),
        f32(nx // 2 + 2, ny // 2 + 2, 8, nz),
        f32(nx // 4 + 2, ny // 4 + 2, 8, nz),
        f32(5, 8, nz),
        f32(4 + sides, 8, nz),
        dma((1,)),
        dma((8,)),
        dma((4 * chunks + 2 * pairs,)),
        f32((2 * (nx + ny) + sides) * bands // 8, 8, nz),
        pltpu.SMEM((bands,), jnp.float32),
        pltpu.SMEM((bands,), jnp.float32),
        f32(nx, ny, nz),
        dma((3,)),
        pltpu.SemaphoreType.REGULAR((2,)),
        f32(bands // 2, nz),
    ]
    filtered = pl.pallas_call(
        functools.partial(kernel, sizes, chunks),
        out_shape=pltpu.VMEM((nx, ny, bands, nz), jnp.float32),
        in_specs=[pl.BlockSpec(memory_space=pltpu.HBM)] * 4,
        out_specs=pl.BlockSpec(memory_space=pltpu.VMEM),
        scratch_shapes=scratch,
        compiler_params=pltpu.CompilerParams(
            collective_id=0, has_side_effects=True, vmem_limit_bytes=48 * 1024 * 1024
        ),
    )(*(pltpu.with_memory_space_constraint(v, pltpu.HBM) for v in (centre, half_width, potential, orbitals)))
    return pl.pallas_call(
        store,
        out_shape=jax.ShapeDtypeStruct(orbitals.shape, jnp.float32),
        in_specs=[pl.BlockSpec(memory_space=pltpu.VMEM)],
        out_specs=pl.BlockSpec(memory_space=pltpu.HBM),
        scratch_shapes=[dma(())],
    )(pltpu.with_memory_space_constraint(filtered, pltpu.VMEM))


def solution(mesh):
    in_specs = (P(None, "gx", "gy", "gz"), P("gx", "gy", "gz"), P(), P())
    out_specs = P(None, "gx", "gy", "gz")
    body = functools.partial(local, dict(mesh.shape), 4)
    return jax.shard_map(body, mesh=mesh, in_specs=in_specs, out_specs=out_specs, check_vma=False)
```

```python
import functools
import math

import jax
import jax.numpy as jnp
from jax import lax
from jax.experimental import pallas as pl
from jax.experimental.pallas import tpu as pltpu
from jax.sharding import PartitionSpec as P

shift_mass = 0.05
jacobi_weight = 2.0 / 3.0
MESH = pl.DeviceIdType.MESH
ORB, FIRST = range(2)


def kernel(sizes, chunks, centre_in, half_width_in, pot_in, orbitals, second, *scratch):
    fine = scratch[0:2]
    one_a, one_b, two_a, two_b, two_c = scratch[2:7]
    zsend, zrecv = scratch[7:9]
    one_edge, one_got, one_halo, two_edge, two_got, last_edge, last_got = scratch[9:16]
    band_a, band_i, pot_b, d1_b, r1_b, r2_b, r_sent, r_got = scratch[16:24]
    load_sem, send_sem, recv_sem, tally = scratch[24:28]
    centre, half_width, pot, small_sem, token, one_c, sum_sent, sum_got = scratch[28:36]
    bands, nx, ny, nz = second.shape[2], second.shape[0], second.shape[1], second.shape[3]
    width = bands // chunks
    groups = width // 8
    pairs = chunks // 2
    early = 1
    mx, my, qx, qy = nx // 2, ny // 2, nx // 4, ny // 4
    sides = 2 if sizes["gz"] > 2 else 1
    at_one = chunks + bands // 8
    at_two = at_one + chunks
    at_last, at_r = at_two + pairs, at_two + 2 * pairs
    at_swept = at_r + 1
    lane = lax.broadcasted_iota(jnp.int32, (8, nz), 1)
    sub = lax.broadcasted_iota(jnp.int32, (8, nz), 0)

    near = {}
    for axis in ("gx", "gy", "gz"):
        me, n = lax.axis_index(axis), sizes[axis]
        near[axis] = (lax.rem(me + n - 1, n), lax.rem(me + 1, n))
    zpeers = [near["gz"][1], near["gz"][0]][:sides]
    gy, ylast = lax.axis_index("gy"), sizes["gy"] - 1
    peers = [{"gx": v} for v in near["gx"]] + [{"gz": v} for v in zpeers]

    def signal(sem, to):
        pl.semaphore_signal(sem, inc=1, device_id=to, device_id_type=MESH)

    barrier = pltpu.get_barrier_semaphore()
    for peer in peers:
        signal(barrier, peer)

    @pl.when(gy > 0)
    def _():
        signal(barrier, {"gy": gy - 1})

    @pl.when(gy < ylast)
    def _():
        signal(barrier, {"gy": gy + 1})

    ycount = lax.div(gy + ylast, ylast + 1) + lax.div(2 * ylast - gy, ylast + 1)

    smalls = [
        pltpu.make_async_copy(src, dst, small_sem.at[j])
        for j, (src, dst) in enumerate(
            [(centre_in, centre), (half_width_in, half_width), (pot_in, pot)]
        )
    ]
    for small in smalls:
        small.start()

    def load(x, c):
        for y in range(ny):
            pltpu.make_async_copy(
                orbitals.at[:, x, y], fine[ORB].at[x + 1, y + 1], load_sem.at[0]
            ).start()
        return c

    lax.fori_loop(0, nx, load, 0)

    def tiles(moves):
        return sum(math.prod(src.shape) for src, _, _ in moves) // (8 * nz)

    def take(n, sem):
        whole = tally.at[pl.ds(0, n)]
        pltpu.make_async_copy(whole, whole, sem).wait()

    def go(moves, sent, got):
        for src, dst, to in moves:
            pltpu.make_async_remote_copy(
                src_ref=src,
                dst_ref=dst,
                send_sem=send_sem.at[sent],
                recv_sem=recv_sem.at[got],
                device_id=to,
                device_id_type=MESH,
            ).start()

    def go_far_first(moves, sent, got):
        downs = [m for m in moves if m[2].get("gy") is near["gy"][0]]
        ups = [m for m in moves if m[2].get("gy") is near["gy"][1]]

        @pl.when(gy == ylast)
        def _():
            go(ups + downs, sent, got)

        @pl.when(gy != ylast)
        def _():
            go(downs + ups, sent, got)

        go([m for m in moves if "gy" not in m[2]], sent, got)

    def arrive(moves, got):
        take(tiles(moves), recv_sem.at[got])

    def leave(moves, times, sent):
        take(times * tiles(moves), send_sem.at[sent])

    def fine_moves(p, k):
        n = (width, 8)[p]
        rows = pl.ds(pl.multiple_of(k * n, 8), n)
        moves = face_moves(fine[p], fine[p], k, n)
        for s, to in enumerate(zpeers):
            moves.append((zsend.at[p, rows], zrecv.at[p, s, rows], {"gz": to}))
        return moves

    def deep_moves(e, edge, got, k):
        ax, ay = e.shape[0] - 4, e.shape[1] - 4
        rows = pl.ds(pl.multiple_of(k * 8, 8), 8)
        ys, xs = pl.ds(2, ay), pl.ds(2, ax)
        lo, hix, hiy, topx, topy = pl.ds(0, 2), pl.ds(ax, 2), pl.ds(ay, 2), pl.ds(ax + 2, 2), pl.ds(ay + 2, 2)
        two = pl.ds(2, 2)
        (xm, xp), (ym, yp) = near["gx"], near["gy"]
        moves = [
            (e.at[xs, two, rows], e.at[xs, topy, rows], {"gy": ym}),
            (e.at[xs, hiy, rows], e.at[xs, lo, rows], {"gy": yp}),
            (e.at[two, ys, rows], e.at[topx, ys, rows], {"gx": xm}),
            (e.at[hix, ys, rows], e.at[lo, ys, rows], {"gx": xp}),
            (e.at[2, 2, rows], e.at[ax + 2, ay + 2, rows], {"gx": xm, "gy": ym}),
            (e.at[ax + 1, 2, rows], e.at[1, ay + 2, rows], {"gx": xp, "gy": ym}),
            (e.at[2, ay + 1, rows], e.at[ax + 2, 1, rows], {"gx": xm, "gy": yp}),
            (e.at[ax + 1, ay + 1, rows], e.at[1, 1, rows], {"gx": xp, "gy": yp}),
        ]
        return edge_moves(edge, got, rows) + moves[4:] + moves[:4]

    def face_moves(src, dst, k, n):
        rows = pl.ds(pl.multiple_of(k * n, 8), n)
        ax, ay = src.shape[0] - 2, src.shape[1] - 2
        ys, xs = pl.ds(1, ay), pl.ds(1, ax)
        (xm, xp), (ym, yp) = near["gx"], near["gy"]
        return [
            (src.at[xs, 1, rows], dst.at[xs, ay + 1, rows], {"gy": ym}),
            (src.at[xs, ay, rows], dst.at[xs, 0, rows], {"gy": yp}),
            (src.at[1, ys, rows], dst.at[ax + 1, ys, rows], {"gx": xm}),
            (src.at[ax, ys, rows], dst.at[0, ys, rows], {"gx": xp}),
        ]

    def edge_moves(edge, got, rows):
        (xm, xp), (ym, yp) = near["gx"], near["gy"]
        spread = [{}, {"gx": xp}, {"gx": xm}, {"gy": yp}, {"gy": ym}]
        return [
            (edge.at[rows], got.at[s, j, rows], {"gz": z, **to})
            for s, z in enumerate(zpeers)
            for j, to in enumerate(spread)
        ]

    def one_cells(k):
        e = one_a
        rows = pl.ds(pl.multiple_of(k * 8, 8), 8)
        (xm, xp), (ym, yp) = near["gx"], near["gy"]
        corners = [
            (e.at[1, 1, rows], e.at[mx + 1, my + 1, rows], {"gx": xm, "gy": ym}),
            (e.at[mx, 1, rows], e.at[0, my + 1, rows], {"gx": xp, "gy": ym}),
            (e.at[1, my, rows], e.at[mx + 1, 0, rows], {"gx": xm, "gy": yp}),
            (e.at[mx, my, rows], e.at[0, 0, rows], {"gx": xp, "gy": yp}),
        ]
        return corners + face_moves(e, e, k, 8)

    def one_extras(k):
        rows = pl.ds(pl.multiple_of(k * 8, 8), 8)
        (xm, xp), (ym, yp) = near["gx"], near["gy"]
        sums = [
            (sum_sent.at[j, rows], sum_got.at[j, rows], to)
            for j, to in ((1, {"gy": ym}), (0, {"gy": yp}), (3, {"gx": xm}), (2, {"gx": xp}))
        ]
        return edge_moves(one_edge, one_got, rows) + sums

    def one_moves(k):
        return one_extras(k)[:5 * sides] + one_cells(k) + one_extras(k)[5 * sides :]

    def swept_moves(k):
        return face_moves(one_b, one_c, k, 8)

    def last_moves(k):
        rows = pl.ds(pl.multiple_of(k * 8, 8), 8)
        moves = face_moves(two_c, two_c, k, 8)
        for s, to in enumerate(zpeers):
            moves.append((last_edge.at[rows], last_got.at[s, rows], {"gz": to}))
        return moves

    def r_moves():
        moves = [
            (r_sent.at[0], r_got.at[1], {"gx": near["gx"][0]}),
            (r_sent.at[1], r_got.at[0], {"gx": near["gx"][1]}),
            (r_sent.at[2], r_got.at[3], {"gy": near["gy"][0]}),
            (r_sent.at[3], r_got.at[2], {"gy": near["gy"][1]}),
        ]
        for s, to in enumerate(zpeers):
            moves.append((r_sent.at[4], r_got.at[4 + s], {"gz": to}))
        return moves

    def two_moves(k):
        return deep_moves(two_a, two_edge, two_got, k)

    def roll(v, shift):
        return pltpu.roll(v, shift % nz, v.ndim - 1)

    def pack(get, ax, ay, w):
        acc = jnp.zeros((8, nz), jnp.float32)
        for x in range(ax):
            for y in range(ay):
                at = 2 * w * (x * ay + y)
                here = (lane >= at) & (lane < at + 2 * w)
                acc = jnp.where(here, roll(get(x, y), at + w), acc)
        return acc

    def edge_at(got, spot, w):
        return roll(got, -(2 * w * spot) - w)

    def join(got, w):
        if sides == 1:
            return got(0)
        return jnp.where((lane & (2 * w - 1)) < w, got(0), got(1))

    def along_z(v, h, w):
        low = roll(jnp.where(lane >= nz - w, h, v), w)
        high = roll(jnp.where(lane < w, h, v), -w)
        return low + high

    def pair_sum(v, w):
        even = (lane & (2 * w - 1)) < w
        return v + jnp.where(even, roll(v, -w), roll(v, w))

    def sweep_edges(own, ends, r, ax, ay, w, coupling):
        cell = w // 2
        mid, xm, xp, ym, yp = ends
        sy, sx = 2 * w, 2 * w * ay
        spot = lane // sy
        yi, xi = spot % ay, spot // ay
        z = jnp.where(
            (lane & (2 * w - 1)) >= w,
            roll(mid, -cell) + roll(own, cell),
            roll(mid, cell) + roll(own, -cell),
        )
        total = z + jnp.where(yi == ay - 1, roll(yp, sy * (ay - 1)), roll(mid, -sy))
        total = total + jnp.where(yi == 0, roll(ym, -sy * (ay - 1)), roll(mid, sy))
        total = total + jnp.where(xi == ax - 1, roll(xp, sx * (ax - 1)), roll(mid, -sx))
        total = total + jnp.where(xi == 0, roll(xm, -sx * (ax - 1)), roll(mid, sx))
        return (2.0 - jacobi_weight) * mid + coupling * r * total

    def sweep_wide(src, dst, ends, r_at, rows, ax, ay, w, coupling):
        mid, xm, xp, ym, yp = ends
        cells = [(x, y, mid, x * ay + y) for x in range(ax) for y in range(ay)]
        cells += [(-1, y, xm, (ax - 1) * ay + y) for y in range(ay)]
        cells += [(ax, y, xp, y) for y in range(ay)]
        cells += [(x, -1, ym, x * ay + ay - 1) for x in range(ax)]
        cells += [(x, ay, yp, x * ay) for x in range(ax)]
        h = (src.shape[0] - ax) // 2
        for x, y, got, spot in cells:
            c = src[x + h, y + h, rows]
            total = along_z(c, edge_at(got, spot, w), w // 2)
            for px, py in ((x - 1, y), (x + 1, y), (x, y - 1), (x, y + 1)):
                if -h <= px < ax + h and -h <= py < ay + h:
                    total = total + src[px + h, py + h, rows]
            dst[x + 1, y + 1, rows] = (2.0 - jacobi_weight) * c + coupling * r_at(x, y) * total

    def total_of(e, x, y, rows, h, w):
        c = e[x + 1, y + 1, rows]
        total = (e[x, y + 1, rows] + e[x + 2, y + 1, rows]) + (
            e[x + 1, y, rows] + e[x + 1, y + 2, rows]
        )
        return c, total + along_z(c, h, w)

    def around(p, sl, got, x):
        e = fine[p]
        c = e[x + 1, pl.ds(1, ny), sl]
        total = e[x, pl.ds(1, ny), sl] + e[x + 2, pl.ds(1, ny), sl]
        total = total + (e[x + 1, pl.ds(0, ny), sl] + e[x + 1, pl.ds(2, ny), sl])
        h = jnp.stack([edge_at(got, x * ny + y, 1) for y in range(ny)])
        low = roll(jnp.where(lane[None] >= nz - 1, h, c), 1)
        high = roll(jnp.where(lane[None] < 1, h, c), -1)
        return c, total + (low + high)

    def fine_edges(p, sl):
        return join(lambda s: zrecv[p, s, sl], 1)

    def fine_pack(p, sl):
        zsend[p, sl] = pack(lambda x, y: fine[p][x + 1, y + 1, sl], nx, ny, 1)

    def slab(k, i):
        return pl.ds(pl.multiple_of(k * width + i * 8, 8), 8)

    pltpu.make_async_copy(
        fine[ORB].at[pl.ds(1, nx), pl.ds(1, ny)],
        fine[ORB].at[pl.ds(1, nx), pl.ds(1, ny)],
        load_sem.at[0],
    ).wait()
    pl.semaphore_wait(barrier, len(peers) + ycount)

    def start_near(k, carry):
        down, up, *rest = fine_moves(ORB, k)

        @pl.when(gy > 0)
        def _():
            go([down], 0, k)

        @pl.when(gy < ylast)
        def _():
            go([up], 0, k)

        go(rest[:2], 0, k)
        return carry

    def start_far(k, carry):
        down, up, *_ = fine_moves(ORB, k)

        @pl.when(gy == 0)
        def _():
            go([down], 0, k)

        @pl.when(gy == ylast)
        def _():
            go([up], 0, k)

        return carry

    lax.fori_loop(0, early, start_near, 0)
    for end, step, sem in ((0, 1, 0), (ylast, -1, 1)):
        first, stop = end + step, ylast - end

        @pl.when((gy != end) & (gy != first))
        def _():
            pl.semaphore_wait(token.at[sem], 1)

        @pl.when((gy != end) & (gy != stop))
        def _():
            signal(token.at[sem], {"gy": gy + step})

    lax.fori_loop(0, early, start_far, 0)

    def start_all(k, carry):
        start_far(k, carry)
        return start_near(k, carry)

    lax.fori_loop(early, chunks, start_all, 0)

    def start_z(k, carry):
        def inner(i, c):
            fine_pack(ORB, slab(k, i))
            return c

        lax.fori_loop(0, groups, inner, 0)
        go(fine_moves(ORB, k)[4:], 0, k)
        return carry

    lax.fori_loop(0, chunks, start_z, 0)

    for small in smalls:
        small.wait()
    for g in range(bands // 8):
        m = jnp.zeros((8, nz), jnp.float32)
        s = jnp.ones((8, nz), jnp.float32)
        for j in range(8):
            m = jnp.where(sub == j, centre[g * 8 + j], m)
            s = jnp.where(sub == j, half_width[g * 8 + j], s)
        band_a[pl.ds(g * 8, 8)] = 3.0 - m
        band_i[pl.ds(g * 8, 8)] = 1.0 / s
    for x in range(nx):
        for y in range(ny):
            pot_b[x, y] = jnp.broadcast_to(pot[x, pl.ds(y, 1), :], (8, nz))
    for x2 in range(qx):
        for y2 in range(qy):
            quad = jnp.zeros((8, nz), jnp.float32)
            for hx in range(2):
                for hy in range(2):
                    x, y = 2 * x2 + hx, 2 * y2 + hy
                    v = pot_b[2 * x, 2 * y] + pot_b[2 * x + 1, 2 * y]
                    v = v + (pot_b[2 * x, 2 * y + 1] + pot_b[2 * x + 1, 2 * y + 1])
                    one = 0.125 * pair_sum(v, 1)
                    quad = quad + one
                    d1 = 0.75 + one + shift_mass
                    d1_b[x, y] = d1
                    r1_b[x + 1, y + 1] = jacobi_weight / d1
            r2_b[x2 + 1, y2 + 1] = jacobi_weight / (0.1875 + 0.125 * pair_sum(quad, 2) + shift_mass)
    for j, (x, y) in enumerate([(0, None), (mx - 1, None), (None, 0), (None, my - 1)]):
        for i in range(my if y is None else mx):
            cx, cy = (x, i) if y is None else (i, y)
            r_sent[j, pl.ds(i, 1)] = r1_b[cx + 1, cy + 1][0:1]
    for j, (x, y) in enumerate([(0, None), (qx - 1, None), (None, 0), (None, qy - 1)]):
        base = my if y is None else mx
        for i in range(qy if y is None else qx):
            cx, cy = (x, i) if y is None else (i, y)
            r_sent[j, pl.ds(base + i, 1)] = r2_b[cx + 1, cy + 1][0:1]
    r_sent[4, pl.ds(0, 1)] = pack(lambda x, y: r1_b[x + 1, y + 1], mx, my, 4)[0:1]
    r_sent[4, pl.ds(1, 1)] = pack(lambda x, y: r2_b[x + 1, y + 1], qx, qy, 8)[0:1]

    go(r_moves(), 6, at_r)

    def step_first(k, carry):
        arrive(fine_moves(ORB, k), k)

        def inner(i, c):
            sl = slab(k, i)
            got = fine_edges(ORB, sl)
            a, f = band_a[sl], band_i[sl]
            for x in range(nx):
                v, total = around(ORB, sl, got, x)
                fine[FIRST][x + 1, pl.ds(1, ny), sl] = ((pot_b[x] + a) * v - 0.5 * total) * f
            fine_pack(FIRST, sl)
            go_far_first(fine_moves(FIRST, k * groups + i), 1, chunks + k * groups + i)
            return c

        lax.fori_loop(0, groups, inner, 0)
        return carry

    lax.fori_loop(0, chunks, step_first, 0)

    arrive(r_moves(), at_r)
    for i in range(my):
        for j, x in ((0, 0), (1, mx + 1)):
            r1_b[x, i + 1] = jnp.broadcast_to(r_got[j, pl.ds(i, 1)], (8, nz))
    for i in range(mx):
        for j, y in ((2, 0), (3, my + 1)):
            r1_b[i + 1, y] = jnp.broadcast_to(r_got[j, pl.ds(i, 1)], (8, nz))
    for i in range(qy):
        for j, x in ((0, 0), (1, qx + 1)):
            r2_b[x, i + 1] = jnp.broadcast_to(r_got[j, pl.ds(my + i, 1)], (8, nz))
    for i in range(qx):
        for j, y in ((2, 0), (3, qy + 1)):
            r2_b[i + 1, y] = jnp.broadcast_to(r_got[j, pl.ds(mx + i, 1)], (8, nz))

    def r_edge(row, w):
        return join(lambda s: jnp.broadcast_to(r_got[4 + s, pl.ds(row, 1)], (8, nz)), w)

    def step_second(k, carry):
        packed = pl.ds(pl.multiple_of(k * 8, 8), 8)

        def inner(i, c):
            arrive(fine_moves(FIRST, k * groups + i), chunks + k * groups + i)
            sl = slab(k, i)
            mine = (lane & 1) == i
            got = fine_edges(FIRST, sl)
            a, f = band_a[sl], 2.0 * band_i[sl]
            for x2 in range(mx):
                both = None
                for x in (2 * x2, 2 * x2 + 1):
                    v, total = around(FIRST, sl, got, x)
                    v = ((pot_b[x] + a) * v - 0.5 * total) * f - fine[ORB][x + 1, pl.ds(1, ny), sl]
                    second[x, :, sl] = v
                    both = v if both is None else both + v
                for y2 in range(my):
                    s = 0.5 * pair_sum(both[2 * y2] + both[2 * y2 + 1], 1)
                    one_a[x2 + 1, y2 + 1, packed] = jnp.where(
                        mine, r1_b[x2 + 1, y2 + 1] * s, one_a[x2 + 1, y2 + 1, packed]
                    )
            return c

        lax.fori_loop(0, groups, inner, 0)
        one_edge[packed] = pack(lambda x, y: one_a[x + 1, y + 1, packed], mx, my, 4)
        for j, outer, inner_cell in (
            (1, lambda i: (i, 0), lambda i: (i, 1)),
            (0, lambda i: (i, my - 1), lambda i: (i, my - 2)),
            (3, lambda i: (0, i), lambda i: (1, i)),
            (2, lambda i: (mx - 1, i), lambda i: (mx - 2, i)),
        ):
            halves = []
            for pair in range(2):
                acc = None
                for i in (2 * pair, 2 * pair + 1):
                    (ox, oy), (ix, iy) = outer(i), inner_cell(i)
                    v = r1_b[ox + 1, oy + 1] * one_a[ix + 1, iy + 1, packed]
                    acc = v if acc is None else acc + v
                halves.append(pair_sum(acc, 2))
            sum_sent[j, packed] = jnp.where((lane & 2) == 0, *halves)
        go_far_first(one_moves(k), 2, at_one + k)
        return carry

    lax.fori_loop(0, chunks, step_second, 0)

    def spread(v, half):
        left = (lane & 2) == 0
        return jnp.where(left, v, roll(v, 2)) if half == 0 else jnp.where(left, roll(v, -2), v)

    def step_residue(k, carry):
        arrive(one_moves(k), at_one + k)
        packed = pl.ds(pl.multiple_of(k * 8, 8), 8)
        rows = pl.ds(pl.multiple_of(lax.div(k, 2) * 8, 8), 8)
        mine = ((lane >> 1) & 1) == lax.rem(k, 2)
        ends = [join(lambda s, j=j: one_got[s, j, packed], 4) for j in range(5)]
        halo = sweep_edges(one_edge[packed], ends, r_edge(0, 4), mx, my, 4, 0.125)
        one_halo[packed] = halo
        sweep_wide(
            one_a, one_b, ends, lambda x, y: r1_b[x + 1, y + 1], packed, mx, my, 4, 0.125
        )
        for x2 in range(qx):
            for y2 in range(qy):
                acc = None
                for x in (2 * x2, 2 * x2 + 1):
                    for y in (2 * y2, 2 * y2 + 1):
                        h = edge_at(halo, x * my + y, 4)
                        c, total = total_of(one_b, x, y, packed, h, 2)
                        d = d1_b[x, y]
                        source = one_a[x + 1, y + 1, packed] * (d * (1.0 / jacobi_weight))
                        v = source - d * c + 0.125 * total
                        acc = v if acc is None else acc + v
                acc = pair_sum(acc, 2)
                for j, near_face, i in ((0, y2 == 0, x2), (1, y2 == qy - 1, x2), (2, x2 == 0, y2), (3, x2 == qx - 1, y2)):
                    if near_face:
                        acc = acc + 0.125**2 * spread(sum_got[j, packed], i)
                s = 0.5 * acc
                two_a[x2 + 2, y2 + 2, rows] = jnp.where(
                    mine, r2_b[x2 + 1, y2 + 1] * s, two_a[x2 + 2, y2 + 2, rows]
                )
        return carry

    def pair_residue(k, carry):
        lax.fori_loop(2 * k, 2 * k + 2, step_residue, 0)
        rows = pl.ds(pl.multiple_of(k * 8, 8), 8)
        two_edge[rows] = pack(lambda x, y: two_a[x + 2, y + 2, rows], qx, qy, 8)
        go_far_first(two_moves(k), 3, at_two + k)
        for half in range(2):
            go_far_first(swept_moves(2 * k + half), 4, at_swept + 2 * k + half)
        return carry

    lax.fori_loop(0, pairs, pair_residue, 0)

    def step_two(k, carry):
        arrive(two_moves(k), at_two + k)
        rows = pl.ds(pl.multiple_of(k * 8, 8), 8)
        ends = [join(lambda s, j=j: two_got[s, j, rows], 8) for j in range(5)]
        halo = sweep_edges(two_edge[rows], ends, r_edge(1, 8), qx, qy, 8, 0.03125)
        sweep_wide(
            two_a, two_b, ends, lambda x, y: r2_b[x + 1, y + 1], rows, qx, qy, 8, 0.03125
        )
        for x in range(qx):
            for y in range(qy):
                c, total = total_of(two_b, x, y, rows, edge_at(halo, x * qy + y, 8), 4)
                two_c[x + 1, y + 1, rows] = (
                    (1.0 - jacobi_weight) * c
                    + two_a[x + 2, y + 2, rows]
                    + 0.03125 * r2_b[x + 1, y + 1] * total
                )
        last_edge[rows] = pack(lambda x, y: two_c[x + 1, y + 1, rows], qx, qy, 4)
        go_far_first(last_moves(k), 5, at_last + k)
        return carry

    lax.fori_loop(0, pairs, step_two, 0)

    def step_last(k, half):
        rows = pl.ds(pl.multiple_of(k * 8, 8), 8)
        packed = pl.ds(pl.multiple_of(k * 16 + half * 8, 8), 8)
        coarse = {}
        for x in range(-1, qx + 1):
            for y in range(-1, qy + 1):
                if 0 <= x < qx or 0 <= y < qy:
                    coarse[x, y] = spread(two_c[x + 1, y + 1, rows], half)
        got = join(lambda s: last_got[s, rows], 4)
        ends = {
            (x, y): spread(edge_at(got, x * qy + y, 4), half) for x in range(qx) for y in range(qy)
        }
        halo = one_halo[packed]

        def at(x, y):
            e = one_b if 0 <= x < mx and 0 <= y < my else one_c
            return e[x + 1, y + 1, packed] + coarse[(x + 2) // 2 - 1, (y + 2) // 2 - 1]

        for x in range(mx):
            for y in range(my):
                c = at(x, y)
                total = (at(x - 1, y) + at(x + 1, y)) + (at(x, y - 1) + at(x, y + 1))
                h = edge_at(halo, x * my + y, 4) + ends[x // 2, y // 2]
                total = total + along_z(c, h, 2)
                v = (1.0 - jacobi_weight) * c + one_a[x + 1, y + 1, packed]
                v = v + 0.125 * r1_b[x + 1, y + 1] * total
                odd = (lane & 1) == 1
                for i, w in enumerate((jnp.where(odd, roll(v, 1), v), jnp.where(odd, v, roll(v, -1)))):
                    sl = slab(2 * k + half, i)
                    for hx in range(2):
                        for hy in range(2):
                            fx, fy = 2 * x + hx, 2 * y + hy
                            second[fx, fy, sl] = second[fx, fy, sl] + w

    def finish(k, carry):
        arrive(last_moves(k), at_last + k)
        for half in range(2):
            arrive(swept_moves(2 * k + half), at_swept + 2 * k + half)
            step_last(k, half)
        return carry

    lax.fori_loop(0, pairs, finish, 0)

    leave(fine_moves(ORB, 0), chunks, 0)
    leave(fine_moves(FIRST, 0), bands // 8, 1)
    leave(one_moves(0), chunks, 2)
    leave(two_moves(0), pairs, 3)
    leave(swept_moves(0), chunks, 4)
    leave(last_moves(0), pairs, 5)
    leave(r_moves(), 1, 6)


def store(filtered, out, sem):
    nx, ny = filtered.shape[:2]

    for x in range(nx):
        for y in range(ny):
            pltpu.make_async_copy(filtered.at[x, y], out.at[:, x, y], sem).start()
    pltpu.make_async_copy(filtered, filtered, sem).wait()


def local(sizes, chunks, orbitals, potential, centre, half_width):
    bands, nx, ny, nz = orbitals.shape
    sides = 2 if sizes["gz"] > 2 else 1
    pairs = chunks // 2

    def f32(*shape):
        return pltpu.VMEM(shape, jnp.float32)

    def padded(cut, halo):
        return f32(nx // cut + 2 * halo, ny // cut + 2 * halo, bands if cut == 1 else bands // cut, nz)

    dma = pltpu.SemaphoreType.DMA
    scratch = [padded(1, 1)] * 2 + [padded(2, 1), padded(2, 1), padded(4, 2), padded(4, 1), padded(4, 1)]
    scratch += [
        f32(2, bands, nz),
        f32(2, sides, bands, nz),
        f32(bands // 2, nz),
        f32(sides, 5, bands // 2, nz),
        f32(bands // 2, nz),
        f32(bands // 4, nz),
        f32(sides, 5, bands // 4, nz),
        f32(bands // 4, nz),
        f32(sides, bands // 4, nz),
        f32(bands, nz),
        f32(bands, nz),
        f32(nx, ny, 8, nz),
        f32(nx // 2, ny // 2, 8, nz),
        f32(nx // 2 + 2, ny // 2 + 2, 8, nz),
        f32(nx // 4 + 2, ny // 4 + 2, 8, nz),
        f32(5, 8, nz),
        f32(4 + sides, 8, nz),
        dma((1,)),
        dma((7,)),
        dma((3 * chunks + bands // 8 + 2 * pairs + 1,)),
        f32((2 * (nx + ny) + sides) * bands // 8, 8, nz),
        pltpu.SMEM((bands,), jnp.float32),
        pltpu.SMEM((bands,), jnp.float32),
        f32(nx, ny, nz),
        dma((3,)),
        pltpu.SemaphoreType.REGULAR((2,)),
        padded(2, 1),
        f32(4, bands // 2, nz),
        f32(4, bands // 2, nz),
    ]
    filtered = pl.pallas_call(
        functools.partial(kernel, sizes, chunks),
        out_shape=pltpu.VMEM((nx, ny, bands, nz), jnp.float32),
        in_specs=[pl.BlockSpec(memory_space=pltpu.HBM)] * 4,
        out_specs=pl.BlockSpec(memory_space=pltpu.VMEM),
        scratch_shapes=scratch,
        compiler_params=pltpu.CompilerParams(
            collective_id=0, has_side_effects=True, vmem_limit_bytes=48 * 1024 * 1024
        ),
    )(*(pltpu.with_memory_space_constraint(v, pltpu.HBM) for v in (centre, half_width, potential, orbitals)))
    return pl.pallas_call(
        store,
        out_shape=jax.ShapeDtypeStruct(orbitals.shape, jnp.float32),
        in_specs=[pl.BlockSpec(memory_space=pltpu.VMEM)],
        out_specs=pl.BlockSpec(memory_space=pltpu.HBM),
        scratch_shapes=[dma(())],
    )(pltpu.with_memory_space_constraint(filtered, pltpu.VMEM))


def solution(mesh):
    in_specs = (P(None, "gx", "gy", "gz"), P("gx", "gy", "gz"), P(), P())
    out_specs = P(None, "gx", "gy", "gz")
    body = functools.partial(local, dict(mesh.shape), 4)
    return jax.shard_map(body, mesh=mesh, in_specs=in_specs, out_specs=out_specs, check_vma=False)
```

```python
import functools
import math

import jax
import jax.numpy as jnp
from jax import lax
from jax.experimental import pallas as pl
from jax.experimental.pallas import tpu as pltpu
from jax.sharding import PartitionSpec as P

shift_mass = 0.05
jacobi_weight = 2.0 / 3.0
MESH = pl.DeviceIdType.MESH
ORB, FIRST = range(2)


def kernel(sizes, chunks, centre_in, half_width_in, pot_in, orbitals, second, *scratch):
    fine = scratch[0:2]
    one_a, one_b, two_a, two_b, two_c = scratch[2:7]
    zsend, zrecv = scratch[7:9]
    one_edge, one_got, one_halo, two_edge, two_got, last_edge, last_got = scratch[9:16]
    band_a, band_i, pot_b, d1_b, r1_b, r2_b, r_sent, r_got = scratch[16:24]
    load_sem, send_sem, recv_sem, tally = scratch[24:28]
    centre, half_width, pot, small_sem, token, one_c, sum_sent, sum_got = scratch[28:36]
    bands, nx, ny, nz = second.shape[2], second.shape[0], second.shape[1], second.shape[3]
    width = bands // chunks
    groups = width // 8
    pairs = chunks // 2
    early = 1
    mx, my, qx, qy = nx // 2, ny // 2, nx // 4, ny // 4
    sides = 2 if sizes["gz"] > 2 else 1
    at_one = chunks + bands // 8
    at_two = at_one + chunks
    at_last, at_r = at_two + pairs, at_two + 2 * pairs
    at_swept = at_r + 1
    lane = lax.broadcasted_iota(jnp.int32, (8, nz), 1)
    sub = lax.broadcasted_iota(jnp.int32, (8, nz), 0)

    near = {}
    for axis in ("gx", "gy", "gz"):
        me, n = lax.axis_index(axis), sizes[axis]
        near[axis] = (lax.rem(me + n - 1, n), lax.rem(me + 1, n))
    zpeers = [near["gz"][1], near["gz"][0]][:sides]
    gy, ylast = lax.axis_index("gy"), sizes["gy"] - 1
    peers = [{"gx": v} for v in near["gx"]] + [{"gz": v} for v in zpeers]

    def signal(sem, to):
        pl.semaphore_signal(sem, inc=1, device_id=to, device_id_type=MESH)

    barrier = pltpu.get_barrier_semaphore()
    for peer in peers:
        signal(barrier, peer)

    @pl.when(gy > 0)
    def _():
        signal(barrier, {"gy": gy - 1})

    @pl.when(gy < ylast)
    def _():
        signal(barrier, {"gy": gy + 1})

    ycount = lax.div(gy + ylast, ylast + 1) + lax.div(2 * ylast - gy, ylast + 1)

    smalls = [
        pltpu.make_async_copy(src, dst, small_sem.at[j])
        for j, (src, dst) in enumerate(
            [(centre_in, centre), (half_width_in, half_width), (pot_in, pot)]
        )
    ]
    for small in smalls:
        small.start()

    def load(x, c):
        for y in range(ny):
            pltpu.make_async_copy(
                orbitals.at[:, x, y], fine[ORB].at[x + 1, y + 1], load_sem.at[0]
            ).start()
        return c

    lax.fori_loop(0, nx, load, 0)

    def tiles(moves):
        return sum(math.prod(src.shape) for src, _, _ in moves) // (8 * nz)

    def take(n, sem):
        whole = tally.at[pl.ds(0, n)]
        pltpu.make_async_copy(whole, whole, sem).wait()

    def go(moves, sent, got):
        for src, dst, to in moves:
            pltpu.make_async_remote_copy(
                src_ref=src,
                dst_ref=dst,
                send_sem=send_sem.at[sent],
                recv_sem=recv_sem.at[got],
                device_id=to,
                device_id_type=MESH,
            ).start()

    def go_far_first(moves, sent, got):
        downs = [m for m in moves if m[2].get("gy") is near["gy"][0]]
        ups = [m for m in moves if m[2].get("gy") is near["gy"][1]]

        @pl.when(gy == ylast)
        def _():
            go(ups + downs, sent, got)

        @pl.when(gy != ylast)
        def _():
            go(downs + ups, sent, got)

        go([m for m in moves if "gy" not in m[2]], sent, got)

    def arrive(moves, got):
        take(tiles(moves), recv_sem.at[got])

    def leave(moves, times, sent):
        take(times * tiles(moves), send_sem.at[sent])

    def fine_moves(p, k):
        n = (width, 8)[p]
        rows = pl.ds(pl.multiple_of(k * n, 8), n)
        moves = face_moves(fine[p], fine[p], k, n)
        for s, to in enumerate(zpeers):
            moves.append((zsend.at[p, rows], zrecv.at[p, s, rows], {"gz": to}))
        return moves

    def deep_moves(e, edge, got, k):
        ax, ay = e.shape[0] - 4, e.shape[1] - 4
        rows = pl.ds(pl.multiple_of(k * 8, 8), 8)
        ys, xs = pl.ds(2, ay), pl.ds(2, ax)
        lo, hix, hiy, topx, topy = pl.ds(0, 2), pl.ds(ax, 2), pl.ds(ay, 2), pl.ds(ax + 2, 2), pl.ds(ay + 2, 2)
        two = pl.ds(2, 2)
        (xm, xp), (ym, yp) = near["gx"], near["gy"]
        moves = [
            (e.at[xs, two, rows], e.at[xs, topy, rows], {"gy": ym}),
            (e.at[xs, hiy, rows], e.at[xs, lo, rows], {"gy": yp}),
            (e.at[two, ys, rows], e.at[topx, ys, rows], {"gx": xm}),
            (e.at[hix, ys, rows], e.at[lo, ys, rows], {"gx": xp}),
            (e.at[2, 2, rows], e.at[ax + 2, ay + 2, rows], {"gx": xm, "gy": ym}),
            (e.at[ax + 1, 2, rows], e.at[1, ay + 2, rows], {"gx": xp, "gy": ym}),
            (e.at[2, ay + 1, rows], e.at[ax + 2, 1, rows], {"gx": xm, "gy": yp}),
            (e.at[ax + 1, ay + 1, rows], e.at[1, 1, rows], {"gx": xp, "gy": yp}),
        ]
        return edge_moves(edge, got, rows) + moves[4:] + moves[:4]

    def face_moves(src, dst, k, n):
        rows = pl.ds(pl.multiple_of(k * n, 8), n)
        ax, ay = src.shape[0] - 2, src.shape[1] - 2
        ys, xs = pl.ds(1, ay), pl.ds(1, ax)
        (xm, xp), (ym, yp) = near["gx"], near["gy"]
        return [
            (src.at[xs, 1, rows], dst.at[xs, ay + 1, rows], {"gy": ym}),
            (src.at[xs, ay, rows], dst.at[xs, 0, rows], {"gy": yp}),
            (src.at[1, ys, rows], dst.at[ax + 1, ys, rows], {"gx": xm}),
            (src.at[ax, ys, rows], dst.at[0, ys, rows], {"gx": xp}),
        ]

    def edge_moves(edge, got, rows):
        (xm, xp), (ym, yp) = near["gx"], near["gy"]
        spread = [{}, {"gx": xp}, {"gx": xm}, {"gy": yp}, {"gy": ym}]
        return [
            (edge.at[rows], got.at[s, j, rows], {"gz": z, **to})
            for s, z in enumerate(zpeers)
            for j, to in enumerate(spread)
        ]

    def one_cells(k):
        e = one_a
        rows = pl.ds(pl.multiple_of(k * 8, 8), 8)
        (xm, xp), (ym, yp) = near["gx"], near["gy"]
        corners = [
            (e.at[1, 1, rows], e.at[mx + 1, my + 1, rows], {"gx": xm, "gy": ym}),
            (e.at[mx, 1, rows], e.at[0, my + 1, rows], {"gx": xp, "gy": ym}),
            (e.at[1, my, rows], e.at[mx + 1, 0, rows], {"gx": xm, "gy": yp}),
            (e.at[mx, my, rows], e.at[0, 0, rows], {"gx": xp, "gy": yp}),
        ]
        return corners + face_moves(e, e, k, 8)

    def one_extras(k):
        rows = pl.ds(pl.multiple_of(k * 8, 8), 8)
        (xm, xp), (ym, yp) = near["gx"], near["gy"]
        sums = [
            (sum_sent.at[j, rows], sum_got.at[j, rows], to)
            for j, to in ((1, {"gy": ym}), (0, {"gy": yp}), (3, {"gx": xm}), (2, {"gx": xp}))
        ]
        return edge_moves(one_edge, one_got, rows) + sums

    def one_moves(k):
        return one_extras(k)[:5 * sides] + one_cells(k) + one_extras(k)[5 * sides :]

    def swept_moves(k):
        return face_moves(one_b, one_c, k, 8)

    def last_moves(k):
        rows = pl.ds(pl.multiple_of(k * 8, 8), 8)
        moves = face_moves(two_c, two_c, k, 8)
        for s, to in enumerate(zpeers):
            moves.append((last_edge.at[rows], last_got.at[s, rows], {"gz": to}))
        return moves

    def r_moves():
        moves = [
            (r_sent.at[0], r_got.at[1], {"gx": near["gx"][0]}),
            (r_sent.at[1], r_got.at[0], {"gx": near["gx"][1]}),
            (r_sent.at[2], r_got.at[3], {"gy": near["gy"][0]}),
            (r_sent.at[3], r_got.at[2], {"gy": near["gy"][1]}),
        ]
        for s, to in enumerate(zpeers):
            moves.append((r_sent.at[4], r_got.at[4 + s], {"gz": to}))
        return moves

    def two_moves(k):
        return deep_moves(two_a, two_edge, two_got, k)

    def roll(v, shift):
        return pltpu.roll(v, shift % nz, v.ndim - 1)

    def pack(get, ax, ay, w):
        acc = jnp.zeros((8, nz), jnp.float32)
        for x in range(ax):
            for y in range(ay):
                at = 2 * w * (x * ay + y)
                here = (lane >= at) & (lane < at + 2 * w)
                acc = jnp.where(here, roll(get(x, y), at + w), acc)
        return acc

    def edge_at(got, spot, w):
        return roll(got, -(2 * w * spot) - w)

    def join(got, w):
        if sides == 1:
            return got(0)
        return jnp.where((lane & (2 * w - 1)) < w, got(0), got(1))

    def along_z(v, h, w):
        low = roll(jnp.where(lane >= nz - w, h, v), w)
        high = roll(jnp.where(lane < w, h, v), -w)
        return low + high

    def pair_sum(v, w):
        even = (lane & (2 * w - 1)) < w
        return v + jnp.where(even, roll(v, -w), roll(v, w))

    def sweep_edges(own, ends, r, ax, ay, w, coupling):
        cell = w // 2
        mid, xm, xp, ym, yp = ends
        sy, sx = 2 * w, 2 * w * ay
        spot = lane // sy
        yi, xi = spot % ay, spot // ay
        z = jnp.where(
            (lane & (2 * w - 1)) >= w,
            roll(mid, -cell) + roll(own, cell),
            roll(mid, cell) + roll(own, -cell),
        )
        total = z + jnp.where(yi == ay - 1, roll(yp, sy * (ay - 1)), roll(mid, -sy))
        total = total + jnp.where(yi == 0, roll(ym, -sy * (ay - 1)), roll(mid, sy))
        total = total + jnp.where(xi == ax - 1, roll(xp, sx * (ax - 1)), roll(mid, -sx))
        total = total + jnp.where(xi == 0, roll(xm, -sx * (ax - 1)), roll(mid, sx))
        return (2.0 - jacobi_weight) * mid + coupling * r * total

    def sweep_wide(src, dst, ends, r_at, rows, ax, ay, w, coupling):
        mid, xm, xp, ym, yp = ends
        cells = [(x, y, mid, x * ay + y) for x in range(ax) for y in range(ay)]
        cells += [(-1, y, xm, (ax - 1) * ay + y) for y in range(ay)]
        cells += [(ax, y, xp, y) for y in range(ay)]
        cells += [(x, -1, ym, x * ay + ay - 1) for x in range(ax)]
        cells += [(x, ay, yp, x * ay) for x in range(ax)]
        h = (src.shape[0] - ax) // 2
        for x, y, got, spot in cells:
            c = src[x + h, y + h, rows]
            total = along_z(c, edge_at(got, spot, w), w // 2)
            for px, py in ((x - 1, y), (x + 1, y), (x, y - 1), (x, y + 1)):
                if -h <= px < ax + h and -h <= py < ay + h:
                    total = total + src[px + h, py + h, rows]
            dst[x + 1, y + 1, rows] = (2.0 - jacobi_weight) * c + coupling * r_at(x, y) * total

    def total_of(e, x, y, rows, h, w):
        c = e[x + 1, y + 1, rows]
        total = (e[x, y + 1, rows] + e[x + 2, y + 1, rows]) + (
            e[x + 1, y, rows] + e[x + 1, y + 2, rows]
        )
        return c, total + along_z(c, h, w)

    def around(p, sl, got, x):
        e = fine[p]
        c = e[x + 1, pl.ds(1, ny), sl]
        total = e[x, pl.ds(1, ny), sl] + e[x + 2, pl.ds(1, ny), sl]
        total = total + (e[x + 1, pl.ds(0, ny), sl] + e[x + 1, pl.ds(2, ny), sl])
        h = jnp.stack([edge_at(got, x * ny + y, 1) for y in range(ny)])
        low = roll(jnp.where(lane[None] >= nz - 1, h, c), 1)
        high = roll(jnp.where(lane[None] < 1, h, c), -1)
        return c, total + (low + high)

    def fine_edges(p, sl):
        return join(lambda s: zrecv[p, s, sl], 1)

    def fine_pack(p, sl):
        zsend[p, sl] = pack(lambda x, y: fine[p][x + 1, y + 1, sl], nx, ny, 1)

    def slab(k, i):
        return pl.ds(pl.multiple_of(k * width + i * 8, 8), 8)

    pltpu.make_async_copy(
        fine[ORB].at[pl.ds(1, nx), pl.ds(1, ny)],
        fine[ORB].at[pl.ds(1, nx), pl.ds(1, ny)],
        load_sem.at[0],
    ).wait()
    pl.semaphore_wait(barrier, len(peers) + ycount)

    def start_near(k, carry):
        down, up, *rest = fine_moves(ORB, k)

        @pl.when(gy > 0)
        def _():
            go([down], 0, k)

        @pl.when(gy < ylast)
        def _():
            go([up], 0, k)

        go(rest[:2], 0, k)
        return carry

    def start_far(k, carry):
        down, up, *_ = fine_moves(ORB, k)

        @pl.when(gy == 0)
        def _():
            go([down], 0, k)

        @pl.when(gy == ylast)
        def _():
            go([up], 0, k)

        return carry

    lax.fori_loop(0, early, start_near, 0)
    for end, step, sem in ((0, 1, 0), (ylast, -1, 1)):
        first, stop = end + step, ylast - end

        @pl.when((gy != end) & (gy != first))
        def _():
            pl.semaphore_wait(token.at[sem], 1)

        @pl.when((gy != end) & (gy != stop))
        def _():
            signal(token.at[sem], {"gy": gy + step})

    lax.fori_loop(0, early, start_far, 0)

    def start_all(k, carry):
        start_far(k, carry)
        return start_near(k, carry)

    lax.fori_loop(early, chunks, start_all, 0)

    def start_z(k, carry):
        def inner(i, c):
            fine_pack(ORB, slab(k, i))
            return c

        lax.fori_loop(0, groups, inner, 0)
        go(fine_moves(ORB, k)[4:], 0, k)
        return carry

    lax.fori_loop(0, chunks, start_z, 0)

    for small in smalls:
        small.wait()
    for g in range(bands // 8):
        m = jnp.zeros((8, nz), jnp.float32)
        s = jnp.ones((8, nz), jnp.float32)
        for j in range(8):
            m = jnp.where(sub == j, centre[g * 8 + j], m)
            s = jnp.where(sub == j, half_width[g * 8 + j], s)
        band_a[pl.ds(g * 8, 8)] = 3.0 - m
        band_i[pl.ds(g * 8, 8)] = 1.0 / s
    for x in range(nx):
        for y in range(ny):
            pot_b[x, y] = jnp.broadcast_to(pot[x, pl.ds(y, 1), :], (8, nz))
    for x2 in range(qx):
        for y2 in range(qy):
            quad = jnp.zeros((8, nz), jnp.float32)
            for hx in range(2):
                for hy in range(2):
                    x, y = 2 * x2 + hx, 2 * y2 + hy
                    v = pot_b[2 * x, 2 * y] + pot_b[2 * x + 1, 2 * y]
                    v = v + (pot_b[2 * x, 2 * y + 1] + pot_b[2 * x + 1, 2 * y + 1])
                    one = 0.125 * pair_sum(v, 1)
                    quad = quad + one
                    d1 = 0.75 + one + shift_mass
                    d1_b[x, y] = d1
                    r1_b[x + 1, y + 1] = jacobi_weight / d1
            r2_b[x2 + 1, y2 + 1] = jacobi_weight / (0.1875 + 0.125 * pair_sum(quad, 2) + shift_mass)
    for j, (x, y) in enumerate([(0, None), (mx - 1, None), (None, 0), (None, my - 1)]):
        for i in range(my if y is None else mx):
            cx, cy = (x, i) if y is None else (i, y)
            r_sent[j, pl.ds(i, 1)] = r1_b[cx + 1, cy + 1][0:1]
    for j, (x, y) in enumerate([(0, None), (qx - 1, None), (None, 0), (None, qy - 1)]):
        base = my if y is None else mx
        for i in range(qy if y is None else qx):
            cx, cy = (x, i) if y is None else (i, y)
            r_sent[j, pl.ds(base + i, 1)] = r2_b[cx + 1, cy + 1][0:1]
    r_sent[4, pl.ds(0, 1)] = pack(lambda x, y: r1_b[x + 1, y + 1], mx, my, 4)[0:1]
    r_sent[4, pl.ds(1, 1)] = pack(lambda x, y: r2_b[x + 1, y + 1], qx, qy, 8)[0:1]

    go(r_moves(), 6, at_r)

    def step_first(k, carry):
        arrive(fine_moves(ORB, k), k)

        def inner(i, c):
            sl = slab(k, i)
            got = fine_edges(ORB, sl)
            a, f = band_a[sl], band_i[sl]
            for x in range(nx):
                v, total = around(ORB, sl, got, x)
                fine[FIRST][x + 1, pl.ds(1, ny), sl] = ((pot_b[x] + a) * v - 0.5 * total) * f
            fine_pack(FIRST, sl)
            go_far_first(fine_moves(FIRST, k * groups + i), 1, chunks + k * groups + i)
            return c

        lax.fori_loop(0, groups, inner, 0)
        return carry

    lax.fori_loop(0, chunks, step_first, 0)

    arrive(r_moves(), at_r)
    for i in range(my):
        for j, x in ((0, 0), (1, mx + 1)):
            r1_b[x, i + 1] = jnp.broadcast_to(r_got[j, pl.ds(i, 1)], (8, nz))
    for i in range(mx):
        for j, y in ((2, 0), (3, my + 1)):
            r1_b[i + 1, y] = jnp.broadcast_to(r_got[j, pl.ds(i, 1)], (8, nz))
    for i in range(qy):
        for j, x in ((0, 0), (1, qx + 1)):
            r2_b[x, i + 1] = jnp.broadcast_to(r_got[j, pl.ds(my + i, 1)], (8, nz))
    for i in range(qx):
        for j, y in ((2, 0), (3, qy + 1)):
            r2_b[i + 1, y] = jnp.broadcast_to(r_got[j, pl.ds(mx + i, 1)], (8, nz))

    def r_edge(row, w):
        return join(lambda s: jnp.broadcast_to(r_got[4 + s, pl.ds(row, 1)], (8, nz)), w)

    def step_second(k, carry):
        packed = pl.ds(pl.multiple_of(k * 8, 8), 8)

        def inner(i, c):
            arrive(fine_moves(FIRST, k * groups + i), chunks + k * groups + i)
            sl = slab(k, i)
            mine = (lane & 1) == i
            got = fine_edges(FIRST, sl)
            a, f = band_a[sl], 2.0 * band_i[sl]
            for x2 in range(mx):
                both = None
                for x in (2 * x2, 2 * x2 + 1):
                    v, total = around(FIRST, sl, got, x)
                    v = ((pot_b[x] + a) * v - 0.5 * total) * f - fine[ORB][x + 1, pl.ds(1, ny), sl]
                    second[x, :, sl] = v
                    both = v if both is None else both + v
                for y2 in range(my):
                    s = 0.5 * pair_sum(both[2 * y2] + both[2 * y2 + 1], 1)
                    one_a[x2 + 1, y2 + 1, packed] = jnp.where(
                        mine, r1_b[x2 + 1, y2 + 1] * s, one_a[x2 + 1, y2 + 1, packed]
                    )
            return c

        lax.fori_loop(0, groups, inner, 0)
        one_edge[packed] = pack(lambda x, y: one_a[x + 1, y + 1, packed], mx, my, 4)
        for j, outer, inner_cell in (
            (1, lambda i: (i, 0), lambda i: (i, 1)),
            (0, lambda i: (i, my - 1), lambda i: (i, my - 2)),
            (3, lambda i: (0, i), lambda i: (1, i)),
            (2, lambda i: (mx - 1, i), lambda i: (mx - 2, i)),
        ):
            halves = []
            for pair in range(2):
                acc = None
                for i in (2 * pair, 2 * pair + 1):
                    (ox, oy), (ix, iy) = outer(i), inner_cell(i)
                    v = r1_b[ox + 1, oy + 1] * one_a[ix + 1, iy + 1, packed]
                    acc = v if acc is None else acc + v
                halves.append(pair_sum(acc, 2))
            sum_sent[j, packed] = jnp.where((lane & 2) == 0, *halves)
        go_far_first(one_moves(k), 2, at_one + k)
        return carry

    lax.fori_loop(0, chunks, step_second, 0)

    def spread(v, half):
        left = (lane & 2) == 0
        return jnp.where(left, v, roll(v, 2)) if half == 0 else jnp.where(left, roll(v, -2), v)

    def step_residue(k, carry):
        arrive(one_moves(k), at_one + k)
        packed = pl.ds(pl.multiple_of(k * 8, 8), 8)
        rows = pl.ds(pl.multiple_of(lax.div(k, 2) * 8, 8), 8)
        mine = ((lane >> 1) & 1) == lax.rem(k, 2)
        ends = [join(lambda s, j=j: one_got[s, j, packed], 4) for j in range(5)]
        halo = sweep_edges(one_edge[packed], ends, r_edge(0, 4), mx, my, 4, 0.125)
        one_halo[packed] = halo
        sweep_wide(
            one_a, one_b, ends, lambda x, y: r1_b[x + 1, y + 1], packed, mx, my, 4, 0.125
        )
        for x2 in range(qx):
            for y2 in range(qy):
                acc = None
                for x in (2 * x2, 2 * x2 + 1):
                    for y in (2 * y2, 2 * y2 + 1):
                        h = edge_at(halo, x * my + y, 4)
                        c, total = total_of(one_b, x, y, packed, h, 2)
                        d = d1_b[x, y]
                        source = one_a[x + 1, y + 1, packed] * (d * (1.0 / jacobi_weight))
                        v = source - d * c + 0.125 * total
                        acc = v if acc is None else acc + v
                acc = pair_sum(acc, 2)
                for j, near_face, i in ((0, y2 == 0, x2), (1, y2 == qy - 1, x2), (2, x2 == 0, y2), (3, x2 == qx - 1, y2)):
                    if near_face:
                        acc = acc + 0.125**2 * spread(sum_got[j, packed], i)
                s = 0.5 * acc
                two_a[x2 + 2, y2 + 2, rows] = jnp.where(
                    mine, r2_b[x2 + 1, y2 + 1] * s, two_a[x2 + 2, y2 + 2, rows]
                )
        return carry

    def pair_residue(k, carry):
        lax.fori_loop(2 * k, 2 * k + 2, step_residue, 0)
        rows = pl.ds(pl.multiple_of(k * 8, 8), 8)
        two_edge[rows] = pack(lambda x, y: two_a[x + 2, y + 2, rows], qx, qy, 8)
        go_far_first(two_moves(k), 3, at_two + k)
        return carry

    lax.fori_loop(0, pairs, pair_residue, 0)
    lax.fori_loop(
        0, chunks, lambda k, c: (go_far_first(swept_moves(k), 4, at_swept + k), c)[1], 0
    )

    def step_two(k, carry):
        arrive(two_moves(k), at_two + k)
        rows = pl.ds(pl.multiple_of(k * 8, 8), 8)
        ends = [join(lambda s, j=j: two_got[s, j, rows], 8) for j in range(5)]
        halo = sweep_edges(two_edge[rows], ends, r_edge(1, 8), qx, qy, 8, 0.03125)
        sweep_wide(
            two_a, two_b, ends, lambda x, y: r2_b[x + 1, y + 1], rows, qx, qy, 8, 0.03125
        )
        for x in range(qx):
            for y in range(qy):
                c, total = total_of(two_b, x, y, rows, edge_at(halo, x * qy + y, 8), 4)
                two_c[x + 1, y + 1, rows] = (
                    (1.0 - jacobi_weight) * c
                    + two_a[x + 2, y + 2, rows]
                    + 0.03125 * r2_b[x + 1, y + 1] * total
                )
        last_edge[rows] = pack(lambda x, y: two_c[x + 1, y + 1, rows], qx, qy, 4)
        go_far_first(last_moves(k), 5, at_last + k)
        return carry

    lax.fori_loop(0, pairs, step_two, 0)

    def step_last(k, half):
        rows = pl.ds(pl.multiple_of(k * 8, 8), 8)
        packed = pl.ds(pl.multiple_of(k * 16 + half * 8, 8), 8)
        coarse = {}
        for x in range(-1, qx + 1):
            for y in range(-1, qy + 1):
                if 0 <= x < qx or 0 <= y < qy:
                    coarse[x, y] = spread(two_c[x + 1, y + 1, rows], half)
        got = join(lambda s: last_got[s, rows], 4)
        ends = {
            (x, y): spread(edge_at(got, x * qy + y, 4), half) for x in range(qx) for y in range(qy)
        }
        halo = one_halo[packed]

        def at(x, y):
            e = one_b if 0 <= x < mx and 0 <= y < my else one_c
            return e[x + 1, y + 1, packed] + coarse[(x + 2) // 2 - 1, (y + 2) // 2 - 1]

        for x in range(mx):
            for y in range(my):
                c = at(x, y)
                total = (at(x - 1, y) + at(x + 1, y)) + (at(x, y - 1) + at(x, y + 1))
                h = edge_at(halo, x * my + y, 4) + ends[x // 2, y // 2]
                total = total + along_z(c, h, 2)
                v = (1.0 - jacobi_weight) * c + one_a[x + 1, y + 1, packed]
                v = v + 0.125 * r1_b[x + 1, y + 1] * total
                odd = (lane & 1) == 1
                for i, w in enumerate((jnp.where(odd, roll(v, 1), v), jnp.where(odd, v, roll(v, -1)))):
                    sl = slab(2 * k + half, i)
                    for hx in range(2):
                        for hy in range(2):
                            fx, fy = 2 * x + hx, 2 * y + hy
                            second[fx, fy, sl] = second[fx, fy, sl] + w

    def finish(k, carry):
        arrive(last_moves(k), at_last + k)
        for half in range(2):
            arrive(swept_moves(2 * k + half), at_swept + 2 * k + half)
            step_last(k, half)
        return carry

    lax.fori_loop(0, pairs, finish, 0)

    leave(fine_moves(ORB, 0), chunks, 0)
    leave(fine_moves(FIRST, 0), bands // 8, 1)
    leave(one_moves(0), chunks, 2)
    leave(two_moves(0), pairs, 3)
    leave(swept_moves(0), chunks, 4)
    leave(last_moves(0), pairs, 5)
    leave(r_moves(), 1, 6)


def store(filtered, out, sem):
    nx, ny = filtered.shape[:2]

    for x in range(nx):
        for y in range(ny):
            pltpu.make_async_copy(filtered.at[x, y], out.at[:, x, y], sem).start()
    pltpu.make_async_copy(filtered, filtered, sem).wait()


def local(sizes, chunks, orbitals, potential, centre, half_width):
    bands, nx, ny, nz = orbitals.shape
    sides = 2 if sizes["gz"] > 2 else 1
    pairs = chunks // 2

    def f32(*shape):
        return pltpu.VMEM(shape, jnp.float32)

    def padded(cut, halo):
        return f32(nx // cut + 2 * halo, ny // cut + 2 * halo, bands if cut == 1 else bands // cut, nz)

    dma = pltpu.SemaphoreType.DMA
    scratch = [padded(1, 1)] * 2 + [padded(2, 1), padded(2, 1), padded(4, 2), padded(4, 1), padded(4, 1)]
    scratch += [
        f32(2, bands, nz),
        f32(2, sides, bands, nz),
        f32(bands // 2, nz),
        f32(sides, 5, bands // 2, nz),
        f32(bands // 2, nz),
        f32(bands // 4, nz),
        f32(sides, 5, bands // 4, nz),
        f32(bands // 4, nz),
        f32(sides, bands // 4, nz),
        f32(bands, nz),
        f32(bands, nz),
        f32(nx, ny, 8, nz),
        f32(nx // 2, ny // 2, 8, nz),
        f32(nx // 2 + 2, ny // 2 + 2, 8, nz),
        f32(nx // 4 + 2, ny // 4 + 2, 8, nz),
        f32(5, 8, nz),
        f32(4 + sides, 8, nz),
        dma((1,)),
        dma((7,)),
        dma((3 * chunks + bands // 8 + 2 * pairs + 1,)),
        f32((2 * (nx + ny) + sides) * bands // 8, 8, nz),
        pltpu.SMEM((bands,), jnp.float32),
        pltpu.SMEM((bands,), jnp.float32),
        f32(nx, ny, nz),
        dma((3,)),
        pltpu.SemaphoreType.REGULAR((2,)),
        padded(2, 1),
        f32(4, bands // 2, nz),
        f32(4, bands // 2, nz),
    ]
    filtered = pl.pallas_call(
        functools.partial(kernel, sizes, chunks),
        out_shape=pltpu.VMEM((nx, ny, bands, nz), jnp.float32),
        in_specs=[pl.BlockSpec(memory_space=pltpu.HBM)] * 4,
        out_specs=pl.BlockSpec(memory_space=pltpu.VMEM),
        scratch_shapes=scratch,
        compiler_params=pltpu.CompilerParams(
            collective_id=0, has_side_effects=True, vmem_limit_bytes=48 * 1024 * 1024
        ),
    )(*(pltpu.with_memory_space_constraint(v, pltpu.HBM) for v in (centre, half_width, potential, orbitals)))
    return pl.pallas_call(
        store,
        out_shape=jax.ShapeDtypeStruct(orbitals.shape, jnp.float32),
        in_specs=[pl.BlockSpec(memory_space=pltpu.VMEM)],
        out_specs=pl.BlockSpec(memory_space=pltpu.HBM),
        scratch_shapes=[dma(())],
    )(pltpu.with_memory_space_constraint(filtered, pltpu.VMEM))


def solution(mesh):
    in_specs = (P(None, "gx", "gy", "gz"), P("gx", "gy", "gz"), P(), P())
    out_specs = P(None, "gx", "gy", "gz")
    body = functools.partial(local, dict(mesh.shape), 4)
    return jax.shard_map(body, mesh=mesh, in_specs=in_specs, out_specs=out_specs, check_vma=False)
```
